256 devices in a mesh: rows: 32 (over y, z), cols: 8 (over x, core).
Axes of the slice: x: 4, y: 4, z: 8, core: 2. Of those that a mesh axis runs over, the one named last changes fastest.
Arguments:
- orthophoto: float32 [3, 4096, 4096], P(None, 'rows', 'cols'), may hold values from 0 to 1
Outputs:
- detail_zero: float32 [3, 4096, 4096], P(None, 'rows', 'cols')
- detail_one: float32 [3, 2048, 2048], P(None, 'rows', 'cols')
- detail_two: float32 [3, 1024, 1024], P(None, 'rows', 'cols')
- detail_three: float32 [3, 512, 512], P(None, 'rows', 'cols')
- detail_four: float32 [3, 256, 256], P(None, 'rows', 'cols')
- coarsest: float32 [3, 128, 128], P(None, 'rows', 'cols')
The draws below stay inside these ranges and needn't reach their ends.
All inputs are finite; a program needn't handle non-finite values.
Results may differ from the reference program's by a relative error of at most 0.00015.
Values sent between devices are 32-bit elements; how exact they have to be, the bound alone decides.
No kernel may reach another device: no remote copies, remote signals or barrier semaphores. Data moves between devices by JAX's collectives and lax.ppermute only.
A program may use at most 64 MiB of HBM per device.

```python
import jax
import jax.numpy as jnp
from jax import lax

CHANNELS = 3
LEVELS = 5
NROWS = 4096
NCOLS = 4096


def steps_of(rng, dims, pieces, least, top_value):
    def one(position, shards_of):
        heights = jax.random.uniform(jax.random.fold_in(jax.random.fold_in(rng, 6), position), (shards_of,), jnp.float32, least / len(pieces), top_value / len(pieces))
        return jnp.repeat(jnp.exp(heights), dims[position] // shards_of).reshape((-1,) + (1,) * (len(dims) - position - 1))

    gain = one(*pieces[0])
    for cut in pieces[1:]:
        gain = gain * one(*cut)
    return gain


def setup_inputs(seed: int = 0) -> dict:
    key_list = jax.random.split(jax.random.key(seed), 2)
    return {
        "orthophoto": jnp.clip(1.0 * jax.random.uniform(key_list[0], (CHANNELS, NROWS, NCOLS), jnp.float32) ** steps_of(key_list[0], (CHANNELS, NROWS, NCOLS), ((1, 32), (2, 8)), -0.2, 0.2), 0.0, 1.0),
    }


TAPS = (0.0625, 0.25, 0.375, 0.25, 0.0625)


def decimate(padded, axis_dim, out_count):
    summed = TAPS[0] * lax.slice_in_dim(padded, 0, 2 * out_count - 1, 2, axis_dim)
    for tap_index in range(1, 5):
        summed = summed + TAPS[tap_index] * lax.slice_in_dim(padded, tap_index, tap_index + 2 * out_count - 1, 2, axis_dim)
    return summed


def shrink(current):
    padded = jnp.pad(current, ((0, 0), (2, 2), (2, 2)), mode="reflect")
    vertical = decimate(padded, 1, current.shape[1] // 2)
    return decimate(vertical, 2, current.shape[2] // 2)


def alternate(even_part, odd_part, axis_dim):
    stacked = jnp.stack([even_part, odd_part], axis=axis_dim + 1)
    new_shape = list(even_part.shape)
    new_shape[axis_dim] = 2 * new_shape[axis_dim]
    return stacked.reshape(new_shape)


def upsample(bordered, axis_dim):
    inner_count = bordered.shape[axis_dim] - 2
    before = lax.slice_in_dim(bordered, 0, inner_count, 1, axis_dim)
    center = lax.slice_in_dim(bordered, 1, inner_count + 1, 1, axis_dim)
    after = lax.slice_in_dim(bordered, 2, inner_count + 2, 1, axis_dim)
    return alternate((before + 6.0 * center + after) * 0.125, (center + after) * 0.5, axis_dim)


def expand(bordered):
    return upsample(upsample(bordered, 1), 2)


def pad_coarse(coarse, axis_dim):
    inner_count = coarse.shape[axis_dim]
    head_cell = lax.slice_in_dim(coarse, 1, 2, 1, axis_dim)
    tail_cell = lax.slice_in_dim(coarse, inner_count - 1, inner_count, 1, axis_dim)
    return jnp.concatenate([head_cell, coarse, tail_cell], axis=axis_dim)


def encode_plane(plane):
    current = plane[None]
    details = []
    for layer_index in range(LEVELS):
        coarse = shrink(current)
        bordered = pad_coarse(pad_coarse(coarse, 1), 2)
        details.append(current - expand(bordered))
        current = coarse
    return (details[0][0], details[1][0], details[2][0], details[3][0], details[4][0], current[0])


def reference(orthophoto):
    results = lax.map(encode_plane, orthophoto)
    return (results[0], results[1], results[2], results[3], results[4], results[5])
```

```python
import functools

import jax
import jax.numpy as jnp
import ml_dtypes
import numpy as np
from jax import lax
from jax.experimental import pallas as pl
from jax.experimental.pallas import tpu as pltpu
from jax.sharding import PartitionSpec as P

LEVELS = 5
F32 = jnp.float32
BF16 = jnp.bfloat16


def reduce_matrix(n):
    pad = np.pad(np.arange(n), (2, 2), mode="reflect")
    out = np.zeros((n // 2, n))
    for j in range(n // 2):
        for s, w in enumerate((1, 4, 6, 4, 1)):
            out[j, pad[2 * j + s]] += w / 16
    return out


def levels_of(n):
    out, total = [], np.eye(n)
    for _ in range(LEVELS):
        total = reduce_matrix(total.shape[0]) @ total
        out.append(total)
    return out


def own_rows(n, which):
    big = levels_of(5 * n)
    out = []
    for level in big:
        m = level.shape[0] // 5
        out.append(np.stack([level[2 * m + j, 2 * n : 3 * n] for j in which(m)]))
    return out


def low_fix(n):
    big, out = levels_of(3 * n), []
    for level, own in zip(big, own_rows(n, lambda m: (-1, 0, 1))):
        assert not level[:2, n:].any()
        out.append(np.stack([level[1, :n], level[0, :n], level[1, :n]]) - own)
    return out


def high_fix(n):
    big, out = levels_of(3 * n), []
    for level, own in zip(big, own_rows(n, lambda m: (m - 1, m))):
        assert not level[-1, : 2 * n].any()
        out.append(np.stack([level[-1, 2 * n :]] * 2) - own)
    return out


def expand_matrix(m):
    out = np.zeros((2 * m, m + 2))
    for i in range(m):
        out[2 * i, i : i + 3] = (0.125, 0.75, 0.125)
        out[2 * i + 1, i + 1 : i + 3] = 0.5
    return out


def exact(matrix, pieces):
    out, rest = [], np.asarray(matrix, np.float64)
    for _ in range(pieces):
        part = rest.astype(ml_dtypes.bfloat16)
        out.append(part)
        rest = rest - part.astype(np.float64)
    assert not rest.any()
    return out


def put(rows, where, count):
    out = np.zeros((count, rows[0].shape[-1]))
    for row, at in zip(rows, where):
        out[at] = row
    return out


OWN_LANE = (0, 256, 384, 448, 480)
LOW_LANE = tuple(496 + k for k in range(LEVELS))
HIGH_LANE = tuple(501 + k for k in range(LEVELS))
ROWS = (72, 40, 24, 16, 8)
ROW_AT = (0, 72, 112, 136, 152)
ROWS_ALL = 160


@functools.lru_cache(None)
def constants(height, width):
    c = {}
    flat = lambda groups: np.concatenate(groups)
    left = flat(own_rows(width, lambda m: (-1, 0)))
    right = flat(own_rows(width, lambda m: (m - 1, m, m + 1)))
    low, high = flat(low_fix(width)), flat(high_fix(width))
    rows = np.zeros((64, width))
    rows[0:10], rows[16:31], rows[32:47], rows[48:58] = left, right, low, high
    c["edge"] = np.concatenate(exact(rows, 2))
    own = np.zeros((width, 512))
    parts = own_rows(width, lambda m: range(-1, m + 1))
    for k, part in enumerate(parts):
        m = part.shape[0] - 2
        own[:, OWN_LANE[k] : OWN_LANE[k] + m] = part[1:-1].T
        own[:, LOW_LANE[k]], own[:, HIGH_LANE[k]] = part[0], part[-1]
    c["col_a"] = exact(own[:, :384], 1)[0]
    c["col_b"] = np.concatenate(exact(own[:, 384:], 2), axis=1)
    land = np.zeros((32, 512))
    for k in range(LEVELS):
        m = width >> (k + 1)
        for q, at in enumerate((LOW_LANE[k], OWN_LANE[k], OWN_LANE[k] + 1)):
            land[3 * k + q, at] = 1
        for q, at in enumerate((OWN_LANE[k] + m - 1, HIGH_LANE[k])):
            land[16 + 2 * k + q, at] = 1
    c["col_land"] = exact(land, 1)[0]
    parts = own_rows(height, lambda m: range(-1, m + 1))
    level_rows = []
    for k, part in enumerate(parts):
        m = part.shape[0] - 2
        level_rows.append(put([*part[1:-1], part[0], part[-1]], range(m + 2), ROWS[k]))
    up, down = own_rows(height, lambda m: (-1, 0)), own_rows(height, lambda m: (m - 1, m, m + 1))
    low, high = low_fix(height), high_fix(height)
    c["row_1"] = exact(np.concatenate([level_rows[0], put([*down[0], *low[0], *up[0], *high[0]], range(10), 16)]), 1)[0]
    c["row_2"] = exact(np.concatenate([level_rows[1], put([*down[1], *low[1], *up[1], *high[1]], range(10), 16)]), 1)[0]
    ends = np.zeros((64, height))
    ends[0:15], ends[16:31], ends[32:42], ends[48:58] = flat(down), flat(low), flat(up), flat(high)
    c["row_3"] = np.concatenate(exact(np.concatenate([*level_rows, ends]), 2))
    land = np.zeros((ROWS_ALL, 48))
    for k in range(LEVELS):
        m = height >> (k + 1)
        for q, at in enumerate((m, 0, 1)):
            land[ROW_AT[k] + at, 3 * k + q] = 1
        for q, at in enumerate((m - 1, m + 1)):
            land[ROW_AT[k] + at, 32 + 2 * k + q] = 1
    c["row_land_3"] = exact(land, 1)[0]
    for name, k, tiles in (("row_land_1", 0, (0, 1)), ("row_land_2", 1, (2,))):
        m = height >> (k + 1)
        for t in tiles:
            land = np.zeros((ROWS[k], 48))
            for q, at in enumerate((m, 0, 1)):
                land[at, 16 + 3 * t + q] = 1
            for q, at in enumerate((m - 1, m + 1)):
                land[at, 42 + 2 * t + q] = 1
            c[f"{name}_{t}"] = exact(land, 1)[0]
    for k in range(LEVELS):
        m = width >> (k + 1)
        e = expand_matrix(m).T
        lanes = np.zeros((512, 2 * m))
        lanes[OWN_LANE[k] : OWN_LANE[k] + m] = e[1:-1]
        lanes[LOW_LANE[k]], lanes[HIGH_LANE[k]] = e[0], e[-1]
        if k == 0:
            lanes = np.concatenate([lanes[:256], lanes[384:]])
        else:
            lanes = lanes[256:] if k == 1 else lanes[384:]
        if k >= 3:
            at = OWN_LANE[k - 1] - 384
            wide = np.zeros((128, 128))
            wide[:, at : at + 2 * m] = lanes
            lanes = wide
        c[f"ecol_{k}"] = exact(lanes, 1)[0]
        m = height >> (k + 1)
        e = expand_matrix(m)
        c[f"erow_{k}"] = exact(np.concatenate([e[:, 1:-1], e[:, :1], e[:, -1:], np.zeros((2 * m, ROWS[k] - m - 2))], axis=1), 1)[0]
    return c


def split(x):
    high = x.astype(BF16)
    rest = x - high.astype(F32)
    middle = rest.astype(BF16)
    return high, middle, (rest - middle.astype(F32)).astype(BF16)


def times(x, matrix):
    return sum(jnp.dot(part, matrix, preferred_element_type=F32) for part in split(x))


def times_left(matrix, x):
    return sum(jnp.dot(matrix, part, preferred_element_type=F32) for part in split(x))


def edge_kernel(x_ref, edge_ref, left_ref, right_ref, low_ref, high_ref):
    for ch in range(x_ref.shape[0]):
        both = sum(
            lax.dot_general(edge_ref[...], part, (((1,), (1,)), ((), ())), preferred_element_type=F32)
            for part in split(x_ref[ch])
        )
        rows = both[:64] + both[64:]
        left_ref[ch], right_ref[ch], low_ref[ch], high_ref[ch] = rows[:16], rows[16:32], rows[32:48], rows[48:]


def column_kernel(x_ref, a_ref, b_ref, u_ref):
    for ch in range(x_ref.shape[0]):
        parts = split(x_ref[ch])
        u_ref[ch, :, :384] = sum(jnp.dot(p, a_ref[...], preferred_element_type=F32) for p in parts)
        last = sum(jnp.dot(p, b_ref[...], preferred_element_type=F32) for p in parts)
        u_ref[ch, :, 384:] = last[:, :128] + last[:, 128:]


def row_kernel(
    u_ref, from_left_ref, from_right_ref, low_ref, high_ref, land_ref, r1_ref, r2_ref, r3_ref,
    t1_ref, t2_ref, t3_ref, down_ref, up_ref, first_ref, last_ref,
):
    col = lax.axis_index("cols")
    is_first, is_last = col == 0, col == lax.axis_size("cols") - 1
    down_ref[...] = jnp.zeros_like(down_ref)
    first_ref[...] = jnp.zeros_like(first_ref)
    for ch in range(u_ref.shape[0]):
        got = jnp.concatenate(
            [
                jnp.where(is_first, low_ref[ch], from_left_ref[ch]),
                jnp.where(is_last, high_ref[ch], from_right_ref[ch]),
            ],
            axis=0,
        )
        v = u_ref[ch] + times(got.T, land_ref[...])
        n1, n2 = ROWS[0], ROWS[1]
        one = times_left(r1_ref[...], v[:, :256])
        two = times_left(r2_ref[...], v[:, 256:384])
        both = times_left(r3_ref[...], v[:, 384:])
        three = both[: ROWS_ALL + 64] + both[ROWS_ALL + 64 :]
        t1_ref[ch] = one[:n1]
        t2_ref[ch] = two[:n2]
        t3_ref[ch] = three[:ROWS_ALL]
        ends = three[ROWS_ALL:]
        for ref, base, at in ((down_ref, 0, 0), (first_ref, 16, 3)):
            ref[ch, 0:16] = ends[base : base + 16]
            ref[ch, 16:19] = one[n1 + at : n1 + at + 3, :128]
            ref[ch, 19:22] = one[n1 + at : n1 + at + 3, 128:]
            ref[ch, 22:25] = two[n2 + at : n2 + at + 3]
        for ref, base, at in ((up_ref, 32, 6), (last_ref, 48, 8)):
            ref[ch, 0:10] = ends[base : base + 10]
            ref[ch, 10:12] = one[n1 + at : n1 + at + 2, :128]
            ref[ch, 12:14] = one[n1 + at : n1 + at + 2, 128:]
            ref[ch, 14:16] = two[n2 + at : n2 + at + 2]


def detail_kernel(
    x_ref, t1_ref, t2_ref, t3_ref, from_up_ref, from_down_ref, first_ref, last_ref,
    l10_ref, l11_ref, l22_ref, l3_ref, ec0, ec1, ec2, ec3, ec4, er0, er1, er2, er3, er4,
    d0_ref, d1_ref, d2_ref, d3_ref, d4_ref, coarsest_ref,
):
    row = lax.axis_index("rows")
    is_first, is_last = row == 0, row == lax.axis_size("rows") - 1
    for ch in range(x_ref.shape[0]):
        got = jnp.concatenate(
            [
                jnp.where(is_first, first_ref[ch], from_up_ref[ch]),
                jnp.where(is_last, last_ref[ch], from_down_ref[ch]),
            ],
            axis=0,
        )
        one = jnp.concatenate(
            [
                t1_ref[ch, :, :128] + times_left(l10_ref[...], got),
                t1_ref[ch, :, 128:] + times_left(l11_ref[...], got),
            ],
            axis=1,
        )
        two = t2_ref[ch] + times_left(l22_ref[...], got)
        three = t3_ref[ch] + times_left(l3_ref[...], got)
        lv = [three[ROW_AT[k] : ROW_AT[k] + ROWS[k]] for k in range(LEVELS)]
        e = times_left(er0[...], times(jnp.concatenate([one, lv[0]], axis=1), ec0[...]))
        d0_ref[ch] = x_ref[ch] - e
        e = times_left(er1[...], times(jnp.concatenate([two, lv[1]], axis=1), ec1[...]))
        d1_ref[ch] = one[: e.shape[0]] - e
        e = times_left(er2[...], times(lv[2], ec2[...]))
        d2_ref[ch] = two[: e.shape[0]] - e
        e = times_left(er3[...], times(lv[3], ec3[...]))
        d3_ref[ch] = (lv[2][: e.shape[0]] - e)[:, :64]
        e = times_left(er4[...], times(lv[4], ec4[...]))
        d4_ref[ch] = (lv[3][: e.shape[0]] - e)[:, 64:96]
        coarsest_ref[ch] = lv[4][:4, 96:112]


def call(kernel, outs, flops, *args):
    bytes_of = lambda a: a.size * a.dtype.itemsize
    outs = [jax.ShapeDtypeStruct(s, F32) for s in outs]
    return pl.pallas_call(
        kernel,
        out_shape=outs,
        in_specs=[pl.BlockSpec(memory_space=pltpu.VMEM)] * len(args),
        out_specs=[pl.BlockSpec(memory_space=pltpu.VMEM)] * len(outs),
        compiler_params=pltpu.CompilerParams(vmem_limit_bytes=24 * 2**20),
        cost_estimate=pl.CostEstimate(
            flops=flops, bytes_accessed=sum(bytes_of(a) for a in args), transcendentals=0
        ),
    )(*args)


def shift(x, axis, step):
    count = lax.axis_size(axis)
    pairs = [(i, i + step) for i in range(count) if 0 <= i + step < count]
    return lax.ppermute(x, axis, pairs)


def body(x):
    channels, height, width = x.shape
    c = {name: jnp.asarray(value) for name, value in constants(height, width).items()}
    side = (channels, 16, height)
    left, right, low, high = call(edge_kernel, [side] * 4, 10**8, x, c["edge"])
    from_left = shift(right, "cols", 1)
    from_right = shift(left, "cols", -1)
    (u,) = call(column_kernel, [(channels, height, 512)], 10**9, x, c["col_a"], c["col_b"])
    t1, t2, t3, down, up, first, last = call(
        row_kernel,
        [(channels, ROWS[0], 256), (channels, ROWS[1], 128), (channels, ROWS_ALL, 128)]
        + [(channels, 32, 128), (channels, 16, 128)] * 2,
        10**8,
        u, from_left, from_right, low, high, c["col_land"], c["row_1"], c["row_2"], c["row_3"],
    )
    from_up = shift(down, "rows", 1)
    from_down = shift(up, "rows", -1)
    outs = [(channels, height >> k, width >> k) for k in range(LEVELS + 1)]
    return call(
        detail_kernel, outs, 10**9,
        x, t1, t2, t3, from_up, from_down, first, last,
        c["row_land_1_0"], c["row_land_1_1"], c["row_land_2_2"], c["row_land_3"],
        *(c[f"ecol_{k}"] for k in range(LEVELS)), *(c[f"erow_{k}"] for k in range(LEVELS)),
    )


def solution(mesh):
    placed = P(None, "rows", "cols")
    return jax.shard_map(
        body, mesh=mesh, in_specs=(placed,), out_specs=(placed,) * 6, check_vma=False
    )
```

```python
import functools

import jax
import jax.numpy as jnp
import ml_dtypes
import numpy as np
from jax import lax
from jax.experimental import pallas as pl
from jax.experimental.pallas import tpu as pltpu
from jax.sharding import PartitionSpec as P

LEVELS = 5
F32 = jnp.float32
BF16 = jnp.bfloat16


def reduce_matrix(n):
    pad = np.pad(np.arange(n), (2, 2), mode="reflect")
    out = np.zeros((n // 2, n))
    for j in range(n // 2):
        for s, w in enumerate((1, 4, 6, 4, 1)):
            out[j, pad[2 * j + s]] += w / 16
    return out


def levels_of(n):
    out, total = [], np.eye(n)
    for _ in range(LEVELS):
        total = reduce_matrix(total.shape[0]) @ total
        out.append(total)
    return out


def own_rows(n, which):
    big = levels_of(5 * n)
    out = []
    for level in big:
        m = level.shape[0] // 5
        out.append(np.stack([level[2 * m + j, 2 * n : 3 * n] for j in which(m)]))
    return out


def low_fix(n):
    big, out = levels_of(3 * n), []
    for level, own in zip(big, own_rows(n, lambda m: (-1, 0, 1))):
        assert not level[:2, n:].any()
        out.append(np.stack([level[1, :n], level[0, :n], level[1, :n]]) - own)
    return out


def high_fix(n):
    big, out = levels_of(3 * n), []
    for level, own in zip(big, own_rows(n, lambda m: (m - 1, m))):
        assert not level[-1, : 2 * n].any()
        out.append(np.stack([level[-1, 2 * n :]] * 2) - own)
    return out


def expand_matrix(m):
    out = np.zeros((2 * m, m + 2))
    for i in range(m):
        out[2 * i, i : i + 3] = (0.125, 0.75, 0.125)
        out[2 * i + 1, i + 1 : i + 3] = 0.5
    return out


def exact(matrix, pieces):
    out, rest = [], np.asarray(matrix, np.float64)
    for _ in range(pieces):
        part = rest.astype(ml_dtypes.bfloat16)
        out.append(part)
        rest = rest - part.astype(np.float64)
    assert not rest.any()
    return out


OWN_LANE = (0, 256, 384, 448, 480)
LOW_LANE = tuple(496 + k for k in range(LEVELS))
HIGH_LANE = tuple(501 + k for k in range(LEVELS))
TILES = ((0, 1, 3), (2, 3), (3,), (3,), (3,))
TILE_LEVELS = (1, 1, 2, 5)
LEAD = 24
TAIL = 32


def rows_of(n):
    return -(-(n + 16) // 8) * 8


@functools.lru_cache(None)
def constants(width):
    c = {}
    left = np.concatenate(own_rows(width, lambda m: (-1, 0)))
    right = np.concatenate(own_rows(width, lambda m: (m - 1, m, m + 1)))
    low, high = np.concatenate(low_fix(width)), np.concatenate(high_fix(width))
    edge = np.zeros((2, 32, 128))
    for side, at, part in ((0, 0, left), (0, 16, low), (1, 0, right), (1, 16, high)):
        near, far = (part[:, :128], part[:, 128:]) if side == 0 else (part[:, -128:], part[:, :-128])
        assert not far.any()
        edge[side, at : at + len(part)] = near
    c["edge"] = np.concatenate(exact(edge, 2), axis=1)
    own = np.zeros((width, 512))
    for k, part in enumerate(own_rows(width, lambda m: range(-1, m + 1))):
        m = part.shape[0] - 2
        own[:, OWN_LANE[k] : OWN_LANE[k] + m] = part[1:-1].T
        own[:, LOW_LANE[k]], own[:, HIGH_LANE[k]] = part[0], part[-1]
    c["col_a"] = exact(own[:, :384], 1)[0]
    c["col_b"] = np.concatenate(exact(own[:, 384:], 2), axis=1)
    land = np.zeros((32, 512))
    for k in range(LEVELS):
        m = width >> (k + 1)
        for q, at in enumerate((LOW_LANE[k], OWN_LANE[k], OWN_LANE[k] + 1)):
            land[3 * k + q, at] = 1
        for q, at in enumerate((OWN_LANE[k] + m - 1, HIGH_LANE[k])):
            land[16 + 2 * k + q, at] = 1
    c["land"] = exact(land, 1)[0]
    for k in range(LEVELS):
        m = width >> (k + 1)
        e = expand_matrix(m).T
        lanes = np.zeros((512, 2 * m))
        lanes[OWN_LANE[k] : OWN_LANE[k] + m] = e[1:-1]
        lanes[LOW_LANE[k]], lanes[HIGH_LANE[k]] = e[0], e[-1]
        if k == 0:
            lanes = np.concatenate([lanes[:256], lanes[384:]])
        else:
            lanes = lanes[256:] if k == 1 else lanes[384:]
        if k >= 3:
            at = OWN_LANE[k - 1] - 384
            wide = np.zeros((128, 128))
            wide[:, at : at + 2 * m] = lanes
            lanes = wide
        c[f"expand_{k}"] = exact(lanes, 1)[0]
    return c


def split(x):
    high = x.astype(BF16)
    rest = x - high.astype(F32)
    middle = rest.astype(BF16)
    return [high, middle, (rest - middle.astype(F32)).astype(BF16)]


def times(x, matrix):
    rows = x.shape[0]
    out = jnp.dot(jnp.concatenate(split(x), axis=0), matrix, preferred_element_type=F32)
    return out[:rows] + out[rows : 2 * rows] + out[2 * rows :]


def edge_kernel(
    x_hbm, edge_hbm, a_hbm, b_hbm, land_hbm,
    send_b_ref, send_a_ref, low_ref, high_ref, x_ref, a_ref, b_ref, land_ref,
    edge_ref, sems,
):
    channels, height, width = x_hbm.shape
    lanes = [pl.ds(0, 128), pl.ds(width - 128, 128), pl.ds(128, width - 256)]
    pairs = [(edge_hbm, edge_ref)] + [(x_hbm.at[:, :, at], x_ref.at[:, :, at]) for at in lanes]
    pairs += [(a_hbm, a_ref), (b_hbm, b_ref), (land_hbm, land_ref)]
    copies = [pltpu.make_async_copy(source, target, sems.at[i]) for i, (source, target) in enumerate(pairs)]
    for copy in copies:
        copy.start()
    for copy in copies[:3]:
        copy.wait()
    odd = lax.axis_index("cols") % 2 == 1
    sides = []
    for side in range(2):
        out = sum(
            lax.dot_general(edge_ref[side], part, (((1,), (1,)), ((), ())), preferred_element_type=F32)
            for part in split(x_ref[:, :, lanes[side].start : lanes[side].start + 128].reshape(channels * height, 128))
        )
        sides.append(out[:32] + out[32:])
    left, right = sides
    for ch in range(channels):
        at = slice(ch * height, (ch + 1) * height)
        send_b_ref[ch] = jnp.where(odd, right[:16, at], left[:16, at])
        send_a_ref[ch] = jnp.where(odd, left[:16, at], right[:16, at])
        low_ref[ch], high_ref[ch] = left[16:, at], right[16:, at]
    for copy in copies[3:]:
        copy.wait()


def column_kernel(x_ref, a_ref, b_ref, u_ref):
    channels, height, width = x_ref.shape
    x = x_ref[...].reshape(channels * height, width)
    u_ref[:, :, :384] = times(x, a_ref[...]).reshape(channels, height, 384)
    last = times(x, b_ref[...])
    u_ref[:, :, 384:] = (last[:, :128] + last[:, 128:]).reshape(channels, height, 128)


def with_row(rows, at, when, new):
    index = lax.broadcasted_iota(jnp.int32, rows.shape, 1)
    return jnp.where((index == at) & when, new, rows)


def row_kernel(
    u_ref, got_b_ref, got_a_ref, low_ref, high_ref, land_ref,
    t1_ref, t2_ref, t3_ref, t4_ref, t5_ref, down_ref, up_ref,
    v_ref, c1_ref, c2_ref, c3_ref, c4_ref,
):
    channels, height = u_ref.shape[0], u_ref.shape[1]
    col, row = lax.axis_index("cols"), lax.axis_index("rows")
    col_odd = col % 2 == 1
    first, last = row == 0, row == lax.axis_size("rows") - 1
    got = []
    for ch in range(channels):
        b, a = got_b_ref[ch], got_a_ref[ch]
        from_left = jnp.where(col == 0, low_ref[ch], jnp.where(col_odd, a, b))
        from_right = jnp.where(col == lax.axis_size("cols") - 1, high_ref[ch], jnp.where(col_odd, b, a))
        got.append(jnp.concatenate([from_left, from_right], axis=0).T)
    landed = times(jnp.concatenate(got, axis=0), land_ref[...])
    chain = (v_ref, c1_ref, c2_ref, c3_ref, c4_ref)
    for k, ref in enumerate(chain):
        n = height >> k
        tiles, size = ref.shape[0], ref.shape[1]
        ref[:, :LEAD] = jnp.zeros((tiles, LEAD, 128), F32)
        ref[:, LEAD + n :] = jnp.zeros((tiles, size - LEAD - n, 128), F32)
    for ch in range(channels):
        for t in range(4):
            lanes = slice(128 * t, 128 * (t + 1))
            v_ref[4 * ch + t, LEAD : LEAD + height] = (
                u_ref[ch, :, lanes] + landed[ch * height : (ch + 1) * height, lanes]
            )
    for tile in range(4 * channels):
        block = v_ref[tile, LEAD - 8 : LEAD]
        index = lax.broadcasted_iota(jnp.int32, block.shape, 0)
        near, far = v_ref[tile, LEAD + 1 : LEAD + 2], v_ref[tile, LEAD + 2 : LEAD + 3]
        v_ref[tile, LEAD - 8 : LEAD] = jnp.where(first, jnp.where(index == 7, near, jnp.where(index == 6, far, block)), block)
        block = v_ref[tile, LEAD + height : LEAD + height + 8]
        near = v_ref[tile, LEAD + height - 2 : LEAD + height - 1]
        v_ref[tile, LEAD + height : LEAD + height + 8] = jnp.where(last & (index == 0), near, block)

    up_ref[...] = jnp.zeros_like(up_ref)
    down_ref[...] = jnp.zeros_like(down_ref)
    lane = lax.broadcasted_iota(jnp.int32, (1, 128), 1) + 384
    tiles_of = ((0, 1, 2, 3), (2, 3), (3,), (3,), (3,))
    outs = (t1_ref, t2_ref, t3_ref, t4_ref, t5_ref)
    for k in range(LEVELS):
        n = height >> (k + 1)
        count = rows_of(n)
        source = chain[k]
        before = tiles_of[k - 1] if k else (0, 1, 2, 3)
        mine = (lane == LOW_LANE[k]) | (lane == HIGH_LANE[k])
        if k >= 2:
            mine = mine | (lane >= OWN_LANE[k]) & (lane < OWN_LANE[k] + (64 >> (k - 2)))
        for ch in range(channels):
            for at, t in enumerate(tiles_of[k]):
                tile = ch * len(before) + before.index(t)
                s = [source[tile, pl.ds(6 + i, count, stride=2), :] for i in range(5)]
                r = (s[0] + s[4]) * 0.0625 + (s[1] + s[3]) * 0.25 + s[2] * 0.375
                index = lax.broadcasted_iota(jnp.int32, r.shape, 0)
                r = jnp.where(first & (index == 7), r[9:10], jnp.where(first & (index == 6), r[10:11], r))
                if k < LEVELS - 1 and TILE_LEVELS[t] > k + 1:
                    onward = jnp.where(last & (index == 8 + n), r[6 + n : 7 + n], r)
                    chain[k + 1][ch * len(tiles_of[k]) + at, LEAD - 8 : LEAD - 8 + count] = onward
                if t in TILES[k]:
                    border = jnp.where(last & (index == 8 + n), r[7 + n : 8 + n], r)
                    outs[k][ch * len(TILES[k]) + TILES[k].index(t)] = border
                    going_up, going_down = r[7:9], r[7 + n : 10 + n]
                    if t == 3:
                        going_up = jnp.where(mine, going_up, 0.0) + (up_ref[ch, 9:11] if k else 0.0)
                        going_down = jnp.where(mine, going_down, 0.0) + (down_ref[ch, 9:12] if k else 0.0)
                    up_ref[ch, 3 * t : 3 * t + 2] = going_up
                    down_ref[ch, 3 * t : 3 * t + 3] = going_down


def detail_kernel(
    x_ref, t1_ref, t2_ref, t3_ref, t4_ref, t5_ref, from_up_ref, from_down_ref, e0, e1, e2, e3, e4,
    d0_hbm, d1_hbm, d2_hbm, d3_hbm, d4_hbm, coarsest_hbm,
    o0, o1, o2, o3, o4, n3, n4, n5, s1, s2, s3, s4, s5, y1, y2, y3, y4, y5, sems,
):
    channels, height = x_ref.shape[0], x_ref.shape[1]
    row = lax.axis_index("rows")
    first, last = row == 0, row == lax.axis_size("rows") - 1
    levels, fines = (s1, s2, s3, s4, s5), (o0, o1, o2, o3, o4)
    hbm = (d0_hbm, d1_hbm, d2_hbm, d3_hbm, d4_hbm)
    for ch in range(channels):
        from_up, from_down = jnp.where(first, 0.0, from_up_ref[ch]), jnp.where(last, 0.0, from_down_ref[ch])
        for k, (t_ref, s_ref) in enumerate(zip((t1_ref, t2_ref, t3_ref, t4_ref, t5_ref), levels)):
            n = height >> (k + 1)
            for at, t in enumerate(TILES[k]):
                tile = ch * len(TILES[k]) + at
                s_ref[tile] = t_ref[tile]
                s_ref[tile, 7:10] = s_ref[tile, 7:10] + from_up[3 * t : 3 * t + 3]
                s_ref[tile, 7 + n : 9 + n] = s_ref[tile, 7 + n : 9 + n] + from_down[3 * t : 3 * t + 2]
    copies = []

    def out(source, target, *at):
        copies.append(pltpu.make_async_copy(source, target, sems.at[at]))
        copies[-1].start()

    for k in range(LEVELS):
        n, count, tiles = height >> (k + 1), levels[k].shape[1], len(TILES[k])
        cells = jnp.concatenate(
            [levels[k][...].reshape(channels, tiles, count, 128)[:, at].reshape(channels * count, 128) for at in range(tiles)],
            axis=1,
        )
        y_ref = (y1, y2, y3, y4, y5)[k]
        y = times(cells, (e0, e1, e2, e3, e4)[k][...])
        y_ref[...] = y.reshape(channels, count, y.shape[1])
        wide = y.shape[1] // 128
        for ch in range(channels):
            for at in range(wide):
                lanes = slice(128 * at, 128 * (at + 1))
                fine = fines[k].at[ch * wide + at]
                if k == 0:
                    fine[...] = x_ref[ch, :, lanes]
                else:
                    fine[...] = levels[k - 1][ch * len(TILES[k - 1]) + at, 8 : 8 + 2 * n]
                before, center, after = (y_ref[ch, i : i + n, lanes] for i in (7, 8, 9))
                fine[pl.ds(0, n, stride=2), :] = fine[pl.ds(0, n, stride=2), :] - (before + 6.0 * center + after) * 0.125
                fine[pl.ds(1, n, stride=2), :] = fine[pl.ds(1, n, stride=2), :] - (center + after) * 0.5
                if k < 3:
                    out(fine, hbm[k].at[ch, :, pl.ds(128 * at, 128)], k, ch, at)
                elif k == 3:
                    n3[ch] = fine[:, :64]
                    out(n3.at[ch], d3_hbm.at[ch], k, ch, 0)
                else:
                    n4[ch] = fine[:, 64:96]
                    out(n4.at[ch], d4_hbm.at[ch], k, ch, 0)
                    n5[ch] = levels[k][ch, 8 : 8 + n, 96:112]
                    out(n5.at[ch], coarsest_hbm.at[ch], k, ch, 1)
    for copy in copies:
        copy.wait()


VMEM = pl.BlockSpec(memory_space=pltpu.VMEM)
HBM = pl.BlockSpec(memory_space=pltpu.HBM)


def call(kernel, outs, flops, args, scratch=(), in_space=VMEM, out_space=VMEM, limit=24 * 2**20):
    bytes_of = lambda a: a.size * a.dtype.itemsize
    outs = [jax.ShapeDtypeStruct(*(s if isinstance(s[0], tuple) else (s, F32))) for s in outs]
    return pl.pallas_call(
        kernel,
        out_shape=outs,
        in_specs=[in_space] * len(args),
        out_specs=[out_space] * len(outs),
        scratch_shapes=list(scratch),
        compiler_params=pltpu.CompilerParams(vmem_limit_bytes=limit),
        cost_estimate=pl.CostEstimate(flops=flops, bytes_accessed=sum(bytes_of(a) for a in args), transcendentals=0),
    )(*args)


def permute(x, axis, to):
    count = lax.axis_size(axis)
    return lax.ppermute(x, axis, [(i, to(i) % count) for i in range(count)])


def body(x):
    channels, height, width = x.shape
    c = {name: jnp.asarray(value) for name, value in constants(width).items()}
    side = (channels, 16, height)
    fixed = [c[name] for name in ("edge", "col_a", "col_b", "land")]
    send_b, send_a, low, high, x_near, col_a, col_b, land = call(
        edge_kernel,
        [side] * 4 + [x.shape] + [(a.shape, BF16) for a in fixed[1:]],
        10**8,
        [pltpu.with_memory_space_constraint(a, pltpu.HBM) for a in (x, *fixed)],
        [pltpu.VMEM(c["edge"].shape, BF16), pltpu.SemaphoreType.DMA((7,))],
        HBM,
    )
    got_b, got_a = permute(send_b, "cols", lambda i: i - 1 + 2 * (i % 2)), permute(send_a, "cols", lambda i: i ^ 1)
    (u,) = call(column_kernel, [(channels, height, 512)], 10**9, (x_near, col_a, col_b))
    ns = [height >> (k + 1) for k in range(LEVELS)]
    tall = lambda tiles, n: pltpu.VMEM((tiles * channels, LEAD + n + TAIL, 128), F32)
    message = (channels, 16, 128)
    *t, down, up = call(
        row_kernel,
        [(channels * len(t), rows_of(n), 128) for n, t in zip(ns, TILES)] + [message] * 2,
        10**8,
        (u, got_b, got_a, low, high, land),
        [tall(4, height), tall(4, ns[0]), tall(2, ns[1]), tall(1, ns[2]), tall(1, ns[3])],
    )
    from_up, from_down = permute(down, "rows", lambda i: i + 1), permute(up, "rows", lambda i: i - 1)
    outs = [(channels, height >> k, width >> k) for k in range(LEVELS + 1)]
    return call(
        detail_kernel,
        outs,
        10**9,
        (x_near, *t, from_up, from_down, *(c[f"expand_{k}"] for k in range(LEVELS))),
        [pltpu.VMEM((channels * max(1, width >> (k + 7)), height >> k, 128), F32) for k in range(LEVELS)]
        + [pltpu.VMEM(s, F32) for s in outs[3:]]
        + [pltpu.VMEM((channels * len(t), rows_of(n), 128), F32) for n, t in zip(ns, TILES)]
        + [pltpu.VMEM((channels, rows_of(n), max(128, width >> k)), F32) for k, n in enumerate(ns)]
        + [pltpu.SemaphoreType.DMA((LEVELS, channels, 4))],
        VMEM,
        HBM,
    )


def solution(mesh):
    placed = P(None, "rows", "cols")
    return jax.shard_map(body, mesh=mesh, in_specs=(placed,), out_specs=(placed,) * 6, check_vma=False)
```

```python
import functools

import jax
import jax.numpy as jnp
import ml_dtypes
import numpy as np
from jax import lax
from jax.experimental import pallas as pl
from jax.experimental.pallas import tpu as pltpu
from jax.sharding import PartitionSpec as P

LEVELS = 5
F32 = jnp.float32
BF16 = jnp.bfloat16


def reduce_matrix(n):
    pad = np.pad(np.arange(n), (2, 2), mode="reflect")
    out = np.zeros((n // 2, n))
    for j in range(n // 2):
        for s, w in enumerate((1, 4, 6, 4, 1)):
            out[j, pad[2 * j + s]] += w / 16
    return out


def levels_of(n):
    out, total = [], np.eye(n)
    for _ in range(LEVELS):
        total = reduce_matrix(total.shape[0]) @ total
        out.append(total)
    return out


def own_rows(n, which):
    big = levels_of(5 * n)
    out = []
    for level in big:
        m = level.shape[0] // 5
        out.append(np.stack([level[2 * m + j, 2 * n : 3 * n] for j in which(m)]))
    return out


def low_fix(n):
    big, out = levels_of(3 * n), []
    for level, own in zip(big, own_rows(n, lambda m: (-1, 0, 1))):
        assert not level[:2, n:].any()
        out.append(np.stack([level[1, :n], level[0, :n], level[1, :n]]) - own)
    return out


def high_fix(n):
    big, out = levels_of(3 * n), []
    for level, own in zip(big, own_rows(n, lambda m: (m - 1, m))):
        assert not level[-1, : 2 * n].any()
        out.append(np.stack([level[-1, 2 * n :]] * 2) - own)
    return out


def expand_matrix(m):
    out = np.zeros((2 * m, m + 2))
    for i in range(m):
        out[2 * i, i : i + 3] = (0.125, 0.75, 0.125)
        out[2 * i + 1, i + 1 : i + 3] = 0.5
    return out


def exact(matrix, pieces):
    out, rest = [], np.asarray(matrix, np.float64)
    for _ in range(pieces):
        part = rest.astype(ml_dtypes.bfloat16)
        out.append(part)
        rest = rest - part.astype(np.float64)
    assert not rest.any()
    return out


OWN_LANE = (0, 256, 384, 448, 480)
LOW_LANE = tuple(496 + k for k in range(LEVELS))
HIGH_LANE = tuple(501 + k for k in range(LEVELS))
COPY_LANE = (506, 507)
TILES = ((0, 1, 3), (2, 3), (3,), (3,), (3,))
TILE_LEVELS = (1, 1, 2, 5)
LEAD = 24
TAIL = 32


def rows_of(n):
    return -(-(n + 16) // 8) * 8


@functools.lru_cache(None)
def constants(width):
    c = {}
    left = np.concatenate(own_rows(width, lambda m: (-1, 0)))
    right = np.concatenate(own_rows(width, lambda m: (m - 1, m, m + 1)))
    low, high = np.concatenate(low_fix(width)), np.concatenate(high_fix(width))
    edge = np.zeros((2, 32, 128))
    for side, at, part in ((0, 0, left), (0, 16, low), (1, 0, right), (1, 16, high)):
        near, far = (part[:, :128], part[:, 128:]) if side == 0 else (part[:, -128:], part[:, :-128])
        assert not far.any()
        edge[side, at : at + len(part)] = near
    c["edge"] = np.concatenate(exact(edge, 2), axis=1)
    own = np.zeros((width, 512))
    for k, part in enumerate(own_rows(width, lambda m: range(-1, m + 1))):
        m = part.shape[0] - 2
        own[:, OWN_LANE[k] : OWN_LANE[k] + m] = part[1:-1].T
        own[:, LOW_LANE[k]], own[:, HIGH_LANE[k]] = part[0], part[-1]
        if k == 0:
            own[:, COPY_LANE[0]], own[:, COPY_LANE[1]] = part[m // 2], part[m // 2 + 1]
    c["col_a"] = exact(own[:, :384], 1)[0]
    c["col_b"] = np.concatenate(exact(own[:, 384:], 2), axis=1)
    land = np.zeros((32, 512))
    for k in range(LEVELS):
        m = width >> (k + 1)
        for q, at in enumerate((LOW_LANE[k], OWN_LANE[k], OWN_LANE[k] + 1)):
            land[3 * k + q, at] = 1
        for q, at in enumerate((OWN_LANE[k] + m - 1, HIGH_LANE[k])):
            land[16 + 2 * k + q, at] = 1
    c["land"] = exact(land, 1)[0]
    third = np.zeros((128, 384))
    for k in range(LEVELS):
        m = width >> (k + 1)
        e = expand_matrix(m).T
        lanes = np.zeros((512, 2 * m))
        lanes[OWN_LANE[k] : OWN_LANE[k] + m] = e[1:-1]
        lanes[LOW_LANE[k]], lanes[HIGH_LANE[k]] = e[0], e[-1]
        if k == 0:
            halves = lanes[:, :m].copy(), lanes[:, m:].copy()
            halves[0][COPY_LANE[1]], halves[1][COPY_LANE[0]] = halves[0][128], halves[1][127]
            c["expand_0"] = np.concatenate([exact(np.concatenate([halves[i][128 * i : 128 * i + 128], halves[i][384:]]), 1)[0] for i in (0, 1)], axis=1)
        elif k == 1:
            c["expand_1"] = exact(lanes[256:], 1)[0]
        else:
            at = 128 * (k - 2) + (OWN_LANE[k - 1] - 384 if k > 2 else 0)
            third[:, at : at + 2 * m] = lanes[384:]
    c["expand_2"] = exact(third, 1)[0]
    return c


def split(x):
    high = x.astype(BF16)
    rest = x - high.astype(F32)
    middle = rest.astype(BF16)
    return [high, middle, (rest - middle.astype(F32)).astype(BF16)]


def times(x, matrix):
    rows = x.shape[0]
    out = jnp.dot(jnp.concatenate(split(x), axis=0), matrix, preferred_element_type=F32)
    return out[:rows] + out[rows : 2 * rows] + out[2 * rows :]


def edge_kernel(
    x_hbm, edge_hbm, a_hbm, b_hbm, land_hbm,
    send_b_ref, send_a_ref, low_ref, high_ref, x_ref, a_ref, b_ref, land_ref,
    edge_ref, sems,
):
    channels, height, width = x_hbm.shape
    tiles = [0, width // 128 - 1, *range(1, width // 128 - 1)]
    pairs = [(edge_hbm, edge_ref)] + [(x_hbm.at[:, :, pl.ds(128 * t, 128)], x_ref.at[:, t]) for t in tiles]
    pairs += [(a_hbm, a_ref), (b_hbm, b_ref), (land_hbm, land_ref)]
    copies = [pltpu.make_async_copy(source, target, sems.at[i]) for i, (source, target) in enumerate(pairs)]
    for copy in copies:
        copy.start()
    for copy in copies[:3]:
        copy.wait()
    odd = lax.axis_index("cols") % 2 == 1
    sides = []
    for side in range(2):
        out = sum(
            lax.dot_general(edge_ref[side], part, (((1,), (1,)), ((), ())), preferred_element_type=F32)
            for part in split(x_ref[:, tiles[side]].reshape(channels * height, 128))
        )
        sides.append(out[:32] + out[32:])
    left, right = sides
    for ch in range(channels):
        at = slice(ch * height, (ch + 1) * height)
        send_b_ref[ch] = jnp.where(odd, right[:16, at], left[:16, at])
        send_a_ref[ch] = jnp.where(odd, left[:16, at], right[:16, at])
        low_ref[ch], high_ref[ch] = left[16:, at], right[16:, at]
    for copy in copies[3:]:
        copy.wait()


def column_kernel(x_ref, a_ref, b_ref, u_ref):
    channels, tiles, height, _ = x_ref.shape
    x = jnp.concatenate([x_ref[:, t].reshape(channels * height, 128) for t in range(tiles)], axis=1)
    u_ref[:, :, :384] = times(x, a_ref[...]).reshape(channels, height, 384)
    last = times(x, b_ref[...])
    u_ref[:, :, 384:] = (last[:, :128] + last[:, 128:]).reshape(channels, height, 128)


def with_row(rows, at, when, new):
    index = lax.broadcasted_iota(jnp.int32, rows.shape, 1)
    return jnp.where((index == at) & when, new, rows)


def row_kernel(
    u_ref, got_b_ref, got_a_ref, low_ref, high_ref, land_ref,
    t1_ref, t2_ref, t3_ref, t4_ref, t5_ref, down_ref, up_ref,
    v_ref, c1_ref, c2_ref, c3_ref, c4_ref,
):
    channels, height = u_ref.shape[0], u_ref.shape[1]
    col, row = lax.axis_index("cols"), lax.axis_index("rows")
    col_odd = col % 2 == 1
    first, last = row == 0, row == lax.axis_size("rows") - 1
    got = []
    for ch in range(channels):
        b, a = got_b_ref[ch], got_a_ref[ch]
        from_left = jnp.where(col == 0, low_ref[ch], jnp.where(col_odd, a, b))
        from_right = jnp.where(col == lax.axis_size("cols") - 1, high_ref[ch], jnp.where(col_odd, b, a))
        got.append(jnp.concatenate([from_left, from_right], axis=0).T)
    landed = times(jnp.concatenate(got, axis=0), land_ref[...])
    chain = (v_ref, c1_ref, c2_ref, c3_ref, c4_ref)
    for k, ref in enumerate(chain):
        n = height >> k
        tiles, size = ref.shape[0], ref.shape[1]
        ref[:, :LEAD] = jnp.zeros((tiles, LEAD, 128), F32)
        ref[:, LEAD + n :] = jnp.zeros((tiles, size - LEAD - n, 128), F32)
    for ch in range(channels):
        for t in range(4):
            lanes = slice(128 * t, 128 * (t + 1))
            v_ref[4 * ch + t, LEAD : LEAD + height] = (
                u_ref[ch, :, lanes] + landed[ch * height : (ch + 1) * height, lanes]
            )
    for tile in range(4 * channels):
        block = v_ref[tile, LEAD - 8 : LEAD]
        index = lax.broadcasted_iota(jnp.int32, block.shape, 0)
        near, far = v_ref[tile, LEAD + 1 : LEAD + 2], v_ref[tile, LEAD + 2 : LEAD + 3]
        v_ref[tile, LEAD - 8 : LEAD] = jnp.where(first, jnp.where(index == 7, near, jnp.where(index == 6, far, block)), block)
        block = v_ref[tile, LEAD + height : LEAD + height + 8]
        near = v_ref[tile, LEAD + height - 2 : LEAD + height - 1]
        v_ref[tile, LEAD + height : LEAD + height + 8] = jnp.where(last & (index == 0), near, block)

    up_ref[...] = jnp.zeros_like(up_ref)
    down_ref[...] = jnp.zeros_like(down_ref)
    lane = lax.broadcasted_iota(jnp.int32, (1, 128), 1) + 384
    tiles_of = ((0, 1, 2, 3), (2, 3), (3,), (3,), (3,))
    outs = (t1_ref, t2_ref, t3_ref, t4_ref, t5_ref)
    for k in range(LEVELS):
        n = height >> (k + 1)
        count = rows_of(n)
        source = chain[k]
        before = tiles_of[k - 1] if k else (0, 1, 2, 3)
        mine = (lane == LOW_LANE[k]) | (lane == HIGH_LANE[k])
        if k == 0:
            mine = mine | (lane == COPY_LANE[0]) | (lane == COPY_LANE[1])
        if k >= 2:
            mine = mine | (lane >= OWN_LANE[k]) & (lane < OWN_LANE[k] + (64 >> (k - 2)))
        for ch in range(channels):
            for at, t in enumerate(tiles_of[k]):
                tile = ch * len(before) + before.index(t)
                s = [source[tile, pl.ds(6 + i, count, stride=2), :] for i in range(5)]
                r = (s[0] + s[4]) * 0.0625 + (s[1] + s[3]) * 0.25 + s[2] * 0.375
                index = lax.broadcasted_iota(jnp.int32, r.shape, 0)
                r = jnp.where(first & (index == 7), r[9:10], jnp.where(first & (index == 6), r[10:11], r))
                if k < LEVELS - 1 and TILE_LEVELS[t] > k + 1:
                    onward = jnp.where(last & (index == 8 + n), r[6 + n : 7 + n], r)
                    chain[k + 1][ch * len(tiles_of[k]) + at, LEAD - 8 : LEAD - 8 + count] = onward
                if t in TILES[k]:
                    border = jnp.where(last & (index == 8 + n), r[7 + n : 8 + n], r)
                    outs[k][ch * len(TILES[k]) + TILES[k].index(t)] = border
                    going_up, going_down = r[7:9], r[7 + n : 10 + n]
                    if t == 3:
                        going_up = jnp.where(mine, going_up, 0.0) + (up_ref[ch, 12:14] if k else 0.0)
                        going_down = jnp.where(mine, going_down, 0.0) + (down_ref[ch, 12:15] if k else 0.0)
                    up_ref[ch, 4 * t : 4 * t + 2] = going_up
                    down_ref[ch, 4 * t : 4 * t + 3] = going_down


def own_kernel(x_ref, t1_ref, t2_ref, t3_ref, t4_ref, t5_ref, e0, e1, e2, g0, g1, g2, g3, g4, y1, y2, y3, y4, y5):
    channels, wide, height, _ = x_ref.shape
    levels, owns, ys = (t1_ref, t2_ref, t3_ref, t4_ref, t5_ref), (g0, g1, g2, g3, g4), (y1, y2, y3, y4, y5)
    for k in range(LEVELS):
        n, count, tiles = height >> (k + 1), levels[k].shape[1], len(TILES[k])
        cells = levels[k][...].reshape(channels, tiles, count, 128)
        cells = [cells[:, at].reshape(channels * count, 128) for at in range(tiles)]
        if k == 0:
            for half in range(2):
                y = times(jnp.concatenate([cells[half], cells[2]], axis=1), e0[:, 256 * half : 256 * half + 256])
                y1[:, :, 256 * half : 256 * half + 256] = y.reshape(channels, count, 256)
        elif k == 1:
            y2[...] = times(jnp.concatenate(cells, axis=1), e1[...]).reshape(y2.shape)
        else:
            ys[k][...] = times(cells[0], e2[:, 128 * (k - 2) : 128 * (k - 1)]).reshape(ys[k].shape)
        across = owns[k].shape[0] // channels
        for ch in range(channels):
            for at in range(across):
                lanes = slice(128 * at, 128 * (at + 1))
                before, center, after = (ys[k][ch, i : i + n, lanes] for i in (7, 8, 9))
                for phase, part in ((0, (before + 6.0 * center + after) * 0.125), (1, (center + after) * 0.5)):
                    if k == 0:
                        fine = x_ref[ch, at, pl.ds(phase, n, stride=2), :]
                    else:
                        fine = levels[k - 1][ch * len(TILES[k - 1]) + at, pl.ds(8 + phase, n, stride=2), :]
                    owns[k][ch * across + at, pl.ds(phase, n, stride=2), :] = fine - part


def end_kernel(
    g0, g1, g2, g3, g4, t5_ref, from_up_ref, from_down_ref, e0, e1, e2,
    d0_hbm, d1_hbm, d2_hbm, d3_hbm, d4_hbm, coarsest_hbm,
    top0, low0, top1, low1, top2, low2, n3, n4, n5, sems,
):
    channels = from_up_ref.shape[0]
    row = lax.axis_index("rows")
    first, last = row == 0, row == lax.axis_size("rows") - 1
    copies = []

    def out(source, target):
        copies.append(pltpu.make_async_copy(source, target, sems.at[len(copies)]))
        copies[-1].start()

    for own, hbm in ((g0, d0_hbm), (g1, d1_hbm), (g2, d2_hbm)):
        across, inner = own.shape[0] // channels, own.shape[1] - 16
        for tile in range(own.shape[0]):
            out(own.at[tile, pl.ds(8, inner)], hbm.at[tile // across, pl.ds(8, inner), pl.ds(128 * (tile % across), 128)])
    r = lax.broadcasted_iota(jnp.int32, (8, 128), 0)

    def weights(*rows):
        out = jnp.zeros((8, 128), F32)
        for at, value in rows:
            out = jnp.where(r == at, value, out)
        return out

    to_top = (weights((0, 0.125)), weights((0, 0.75), (1, 0.5), (2, 0.125)), weights((0, 0.125), (1, 0.5), (2, 0.75), (3, 0.5), (4, 0.125)))
    to_low = (weights((4, 0.125), (5, 0.5), (6, 0.75), (7, 0.5)), weights((6, 0.125), (7, 0.5)))
    coarse, fine = [[] for _ in range(4)], []
    for ch in range(channels):
        fine.append([])
        for t in range(4):
            up = jnp.where(first, 0.0, from_up_ref[ch, 4 * t : 4 * t + 3])
            down = jnp.where(last, 0.0, from_down_ref[ch, 4 * t : 4 * t + 2])
            coarse[t].append(sum(w * up[i : i + 1] for i, w in enumerate(to_top)))
            coarse[t].append(sum(w * down[i : i + 1] for i, w in enumerate(to_low)))
            fine[ch].append(
                (jnp.where(r == 0, up[1:2], jnp.where(r == 1, up[2:3], 0.0)), jnp.where(r == 7, down[:1], 0.0), down[:1])
            )
    coarse = [jnp.concatenate(tiles, axis=0) for tiles in coarse]
    e = [times(jnp.concatenate([coarse[half], coarse[3]], axis=1), e0[:, 256 * half : 256 * half + 256]) for half in range(2)]
    e.append(times(jnp.concatenate([coarse[2], coarse[3]], axis=1), e1[...]))
    e.append(times(coarse[3], e2[...]))
    for ch in range(channels):
        top, low = slice(16 * ch, 16 * ch + 8), slice(16 * ch + 8, 16 * ch + 16)
        for t in range(4):
            lanes, part = slice(128 * t, 128 * (t + 1)), e[t // 2][:, 128 * (t % 2) : 128 * (t % 2) + 128]
            top0[ch, :, lanes] = g0[4 * ch + t, :8] - part[top]
            low0[ch, :, lanes] = g0[4 * ch + t, -8:] - part[low]
        for t in range(2):
            lanes = slice(128 * t, 128 * (t + 1))
            top1[ch, :, lanes] = g1[2 * ch + t, :8] + fine[ch][t][0] - e[2][top, lanes]
            low1[ch, :, lanes] = g1[2 * ch + t, -8:] + fine[ch][t][1] - e[2][low, lanes]
        top2[ch] = g2[ch, :8] + fine[ch][2][0] - e[3][top, :128]
        low2[ch] = g2[ch, -8:] + fine[ch][2][1] - e[3][low, :128]
        n3[ch, :8] = (g3[ch, :8] + fine[ch][3][0] - e[3][top, 128:256])[:, :64]
        n3[ch, 8:] = (g3[ch, 8:] + fine[ch][3][1] - e[3][low, 128:256])[:, :64]
        n4[ch] = (g4[ch] + fine[ch][3][0] + fine[ch][3][1] - e[3][top, 256:] - e[3][low, 256:])[:, 64:96]
        n5[ch] = (t5_ref[ch, 8:16] + fine[ch][3][0] + jnp.where(r == 3, fine[ch][3][2], 0.0))[:4, 96:112]
    for top, low, hbm in ((top0, low0, d0_hbm), (top1, low1, d1_hbm), (top2, low2, d2_hbm)):
        out(top, hbm.at[:, pl.ds(0, 8)])
        out(low, hbm.at[:, pl.ds(hbm.shape[1] - 8, 8)])
    out(n3, d3_hbm)
    out(n4, d4_hbm)
    out(n5, coarsest_hbm)
    for copy in copies:
        copy.wait()


VMEM = pl.BlockSpec(memory_space=pltpu.VMEM)
HBM = pl.BlockSpec(memory_space=pltpu.HBM)


def call(kernel, outs, flops, args, scratch=(), in_space=VMEM, out_space=VMEM, limit=24 * 2**20):
    bytes_of = lambda a: a.size * a.dtype.itemsize
    outs = [jax.ShapeDtypeStruct(*(s if isinstance(s[0], tuple) else (s, F32))) for s in outs]
    return pl.pallas_call(
        kernel,
        out_shape=outs,
        in_specs=[in_space] * len(args),
        out_specs=[out_space] * len(outs),
        scratch_shapes=list(scratch),
        compiler_params=pltpu.CompilerParams(vmem_limit_bytes=limit),
        cost_estimate=pl.CostEstimate(flops=flops, bytes_accessed=sum(bytes_of(a) for a in args), transcendentals=0),
    )(*args)


def permute(x, axis, to):
    count = lax.axis_size(axis)
    return lax.ppermute(x, axis, [(i, to(i) % count) for i in range(count)])


def body(x):
    channels, height, width = x.shape
    c = {name: jnp.asarray(value) for name, value in constants(width).items()}
    side = (channels, 16, height)
    fixed = [c[name] for name in ("edge", "col_a", "col_b", "land")]
    send_b, send_a, low, high, x_near, col_a, col_b, land = call(
        edge_kernel,
        [side] * 4 + [(channels, width // 128, height, 128)] + [(a.shape, BF16) for a in fixed[1:]],
        10**8,
        [pltpu.with_memory_space_constraint(a, pltpu.HBM) for a in (x, *fixed)],
        [pltpu.VMEM(c["edge"].shape, BF16), pltpu.SemaphoreType.DMA((8,))],
        HBM,
    )
    got_b, got_a = permute(send_b, "cols", lambda i: i - 1 + 2 * (i % 2)), permute(send_a, "cols", lambda i: i ^ 1)
    (u,) = call(column_kernel, [(channels, height, 512)], 10**9, (x_near, col_a, col_b))
    ns = [height >> (k + 1) for k in range(LEVELS)]
    tall = lambda tiles, n: pltpu.VMEM((tiles * channels, LEAD + n + TAIL, 128), F32)
    message = (channels, 16, 128)
    *t, down, up = call(
        row_kernel,
        [(channels * len(t), rows_of(n), 128) for n, t in zip(ns, TILES)] + [message] * 2,
        10**8,
        (u, got_b, got_a, low, high, land),
        [tall(4, height), tall(4, ns[0]), tall(2, ns[1]), tall(1, ns[2]), tall(1, ns[3])],
    )
    from_up, from_down = permute(down, "rows", lambda i: i + 1), permute(up, "rows", lambda i: i - 1)
    expand = [c[f"expand_{k}"] for k in range(3)]
    own = call(
        own_kernel,
        [(channels * max(1, width >> (k + 7)), height >> k, 128) for k in range(LEVELS)],
        10**9,
        (x_near, *t, *expand),
        [pltpu.VMEM((channels, rows_of(n), max(128, width >> k)), F32) for k, n in enumerate(ns)],
    )
    outs = [(channels, height >> k, width >> k) for k in range(LEVELS + 1)]
    return call(
        end_kernel,
        outs,
        10**8,
        (*own, t[-1], from_up, from_down, *expand),
        [pltpu.VMEM((channels, 8, s[2]), F32) for s in outs[:3] for _ in range(2)]
        + [pltpu.VMEM(s, F32) for s in outs[3:]]
        + [pltpu.SemaphoreType.DMA((30,))],
        VMEM,
        HBM,
    )


def solution(mesh):
    placed = P(None, "rows", "cols")
    return jax.shard_map(body, mesh=mesh, in_specs=(placed,), out_specs=(placed,) * 6, check_vma=False)
```

```python
import functools

import jax
import jax.numpy as jnp
import ml_dtypes
import numpy as np
from jax import lax
from jax.experimental import pallas as pl
from jax.experimental.pallas import tpu as pltpu
from jax.sharding import PartitionSpec as P


LEVELS = 5
F32 = jnp.float32
BF16 = jnp.bfloat16


def reduce_matrix(n):
    pad = np.pad(np.arange(n), (2, 2), mode="reflect")
    out = np.zeros((n // 2, n))
    for j in range(n // 2):
        for s, w in enumerate((1, 4, 6, 4, 1)):
            out[j, pad[2 * j + s]] += w / 16
    return out


def levels_of(n):
    out, total = [], np.eye(n)
    for _ in range(LEVELS):
        total = reduce_matrix(total.shape[0]) @ total
        out.append(total)
    return out


def own_rows(n, which):
    big = levels_of(5 * n)
    out = []
    for level in big:
        m = level.shape[0] // 5
        out.append(np.stack([level[2 * m + j, 2 * n : 3 * n] for j in which(m)]))
    return out


def low_fix(n):
    big, out = levels_of(3 * n), []
    for level, own in zip(big, own_rows(n, lambda m: (-1, 0, 1))):
        assert not level[:2, n:].any()
        out.append(np.stack([level[1, :n], level[0, :n], level[1, :n]]) - own)
    return out


def high_fix(n):
    big, out = levels_of(3 * n), []
    for level, own in zip(big, own_rows(n, lambda m: (m - 1, m))):
        assert not level[-1, : 2 * n].any()
        out.append(np.stack([level[-1, 2 * n :]] * 2) - own)
    return out


def expand_matrix(m):
    out = np.zeros((2 * m, m + 2))
    for i in range(m):
        out[2 * i, i : i + 3] = (0.125, 0.75, 0.125)
        out[2 * i + 1, i + 1 : i + 3] = 0.5
    return out


def exact(matrix, pieces):
    out, rest = [], np.asarray(matrix, np.float64)
    for _ in range(pieces):
        part = rest.astype(ml_dtypes.bfloat16)
        out.append(part)
        rest = rest - part.astype(np.float64)
    assert not rest.any()
    return out


OWN_LANE = (0, 256, 384, 448, 480)
LOW_LANE = tuple(496 + k for k in range(LEVELS))
HIGH_LANE = tuple(501 + k for k in range(LEVELS))
COPY_LANE = (506, 507)
TILES = ((0, 1, 3), (2, 3), (3,), (3,), (3,))
TILE_LEVELS = (1, 1, 2, 5)
LEAD = 24
TAIL = 32


def rows_of(n):
    return -(-(n + 16) // 8) * 8


@functools.lru_cache(None)
def constants(width):
    c = {}
    left = np.concatenate(own_rows(width, lambda m: (-1, 0)))
    right = np.concatenate(own_rows(width, lambda m: (m - 1, m, m + 1)))
    low, high = np.concatenate(low_fix(width)), np.concatenate(high_fix(width))
    edge = np.zeros((2, 32, 128))
    for side, at, part in ((0, 0, left), (0, 16, low), (1, 0, right), (1, 16, high)):
        near, far = (part[:, :128], part[:, 128:]) if side == 0 else (part[:, -128:], part[:, :-128])
        assert not far.any()
        edge[side, at : at + len(part)] = near
    c["edge"] = np.concatenate(exact(edge, 2), axis=1)
    own = np.zeros((width, 512))
    for k, part in enumerate(own_rows(width, lambda m: range(-1, m + 1))):
        m = part.shape[0] - 2
        own[:, OWN_LANE[k] : OWN_LANE[k] + m] = part[1:-1].T
        own[:, LOW_LANE[k]], own[:, HIGH_LANE[k]] = part[0], part[-1]
        if k == 0:
            own[:, COPY_LANE[0]], own[:, COPY_LANE[1]] = part[m // 2], part[m // 2 + 1]
    c["col_a"] = exact(own[:, :384], 1)[0]
    c["col_b"] = np.concatenate(exact(own[:, 384:], 2), axis=1)
    land = np.zeros((32, 512))
    for k in range(LEVELS):
        m = width >> (k + 1)
        for q, at in enumerate((LOW_LANE[k], OWN_LANE[k], OWN_LANE[k] + 1)):
            land[3 * k + q, at] = 1
        for q, at in enumerate((OWN_LANE[k] + m - 1, HIGH_LANE[k])):
            land[16 + 2 * k + q, at] = 1
    c["land"] = exact(land, 1)[0]
    third = np.zeros((128, 384))
    for k in range(LEVELS):
        m = width >> (k + 1)
        e = expand_matrix(m).T
        lanes = np.zeros((512, 2 * m))
        lanes[OWN_LANE[k] : OWN_LANE[k] + m] = e[1:-1]
        lanes[LOW_LANE[k]], lanes[HIGH_LANE[k]] = e[0], e[-1]
        if k == 0:
            halves = lanes[:, :m].copy(), lanes[:, m:].copy()
            halves[0][COPY_LANE[1]], halves[1][COPY_LANE[0]] = halves[0][128], halves[1][127]
            c["expand_0"] = np.concatenate([exact(np.concatenate([halves[i][128 * i : 128 * i + 128], halves[i][384:]]), 1)[0] for i in (0, 1)], axis=1)
        elif k == 1:
            c["expand_1"] = exact(lanes[256:], 1)[0]
        else:
            at = 128 * (k - 2) + (OWN_LANE[k - 1] - 384 if k > 2 else 0)
            third[:, at : at + 2 * m] = lanes[384:]
    c["expand_2"] = exact(third, 1)[0]
    return c


def split(x):
    high = x.astype(BF16)
    rest = x - high.astype(F32)
    middle = rest.astype(BF16)
    return [high, middle, (rest - middle.astype(F32)).astype(BF16)]


def times(x, matrix):
    rows = x.shape[0]
    out = jnp.dot(jnp.concatenate(split(x), axis=0), matrix, preferred_element_type=F32)
    return out[:rows] + out[rows : 2 * rows] + out[2 * rows :]


def edge_kernel(
    x_hbm, edge_hbm, a_hbm, b_hbm, land_hbm,
    send_b_ref, send_a_ref, low_ref, high_ref, x_ref, a_ref, b_ref, land_ref,
    edge_ref, sems,
):
    channels, height, width = x_hbm.shape
    tiles = [0, width // 128 - 1, *range(1, width // 128 - 1)]
    pairs = [(edge_hbm, edge_ref)] + [(x_hbm.at[:, :, pl.ds(128 * t, 128)], x_ref.at[:, t]) for t in tiles]
    pairs += [(a_hbm, a_ref), (b_hbm, b_ref), (land_hbm, land_ref)]
    copies = [pltpu.make_async_copy(source, target, sems.at[i]) for i, (source, target) in enumerate(pairs)]
    for copy in copies:
        copy.start()
    for copy in copies[:3]:
        copy.wait()
    odd = lax.axis_index("cols") % 2 == 1
    sides = []
    for side in range(2):
        out = sum(
            lax.dot_general(edge_ref[side], part, (((1,), (1,)), ((), ())), preferred_element_type=F32)
            for part in split(x_ref[:, tiles[side]].reshape(channels * height, 128))
        )
        sides.append(out[:32] + out[32:])
    left, right = sides
    for ch in range(channels):
        at = slice(ch * height, (ch + 1) * height)
        send_b_ref[ch] = jnp.where(odd, right[:16, at], left[:16, at])
        send_a_ref[ch] = jnp.where(odd, left[:16, at], right[:16, at])
        low_ref[ch], high_ref[ch] = left[16:, at], right[16:, at]
    for copy in copies[3:]:
        copy.wait()


def column_kernel(x_ref, a_ref, b_ref, u_ref):
    channels, tiles, height, _ = x_ref.shape
    x = jnp.concatenate([x_ref[:, t].reshape(channels * height, 128) for t in range(tiles)], axis=1)
    u_ref[:, :, :384] = times(x, a_ref[...]).reshape(channels, height, 384)
    last = times(x, b_ref[...])
    u_ref[:, :, 384:] = (last[:, :128] + last[:, 128:]).reshape(channels, height, 128)


def row_kernel(
    u_ref, got_b_ref, got_a_ref, low_ref, high_ref, land_ref,
    t1_ref, t2_ref, t3_ref, t4_ref, t5_ref, send_b_ref, send_a_ref,
    v_ref, c1_ref, c2_ref, c3_ref, c4_ref, up_ref, down_ref,
):
    channels, height = u_ref.shape[0], u_ref.shape[1]
    col, row = lax.axis_index("cols"), lax.axis_index("rows")
    col_odd = col % 2 == 1
    row_odd, first, last = row % 2 == 1, row == 0, row == lax.axis_size("rows") - 1
    got = []
    for ch in range(channels):
        b, a = got_b_ref[ch], got_a_ref[ch]
        from_left = jnp.where(col == 0, low_ref[ch], jnp.where(col_odd, a, b))
        from_right = jnp.where(col == lax.axis_size("cols") - 1, high_ref[ch], jnp.where(col_odd, b, a))
        got.append(jnp.concatenate([from_left, from_right], axis=0).T)
    landed = times(jnp.concatenate(got, axis=0), land_ref[...])
    chain = (v_ref, c1_ref, c2_ref, c3_ref, c4_ref)
    for k, ref in enumerate(chain):
        n = height >> k
        tiles, size = ref.shape[0], ref.shape[1]
        ref[:, :LEAD] = jnp.zeros((tiles, LEAD, 128), F32)
        ref[:, LEAD + n :] = jnp.zeros((tiles, size - LEAD - n, 128), F32)
    for ch in range(channels):
        for t in range(4):
            lanes = slice(128 * t, 128 * (t + 1))
            v_ref[4 * ch + t, LEAD : LEAD + height] = (
                u_ref[ch, :, lanes] + landed[ch * height : (ch + 1) * height, lanes]
            )
    for tile in range(4 * channels):
        block = v_ref[tile, LEAD - 8 : LEAD]
        index = lax.broadcasted_iota(jnp.int32, block.shape, 0)
        near, far = v_ref[tile, LEAD + 1 : LEAD + 2], v_ref[tile, LEAD + 2 : LEAD + 3]
        v_ref[tile, LEAD - 8 : LEAD] = jnp.where(first, jnp.where(index == 7, near, jnp.where(index == 6, far, block)), block)
        block = v_ref[tile, LEAD + height : LEAD + height + 8]
        near = v_ref[tile, LEAD + height - 2 : LEAD + height - 1]
        v_ref[tile, LEAD + height : LEAD + height + 8] = jnp.where(last & (index == 0), near, block)

    up_ref[...] = jnp.zeros_like(up_ref)
    down_ref[...] = jnp.zeros_like(down_ref)
    lane = lax.broadcasted_iota(jnp.int32, (1, 128), 1) + 384
    tiles_of = ((0, 1, 2, 3), (2, 3), (3,), (3,), (3,))
    outs = (t1_ref, t2_ref, t3_ref, t4_ref, t5_ref)
    for k in range(LEVELS):
        n = height >> (k + 1)
        count = rows_of(n)
        source = chain[k]
        before = tiles_of[k - 1] if k else (0, 1, 2, 3)
        mine = (lane == LOW_LANE[k]) | (lane == HIGH_LANE[k])
        if k == 0:
            mine = mine | (lane == COPY_LANE[0]) | (lane == COPY_LANE[1])
        if k >= 2:
            mine = mine | (lane >= OWN_LANE[k]) & (lane < OWN_LANE[k] + (64 >> (k - 2)))
        for ch in range(channels):
            for at, t in enumerate(tiles_of[k]):
                tile = ch * len(before) + before.index(t)
                s = [source[tile, pl.ds(6 + i, count, stride=2), :] for i in range(5)]
                r = (s[0] + s[4]) * 0.0625 + (s[1] + s[3]) * 0.25 + s[2] * 0.375
                index = lax.broadcasted_iota(jnp.int32, r.shape, 0)
                r = jnp.where(first & (index == 7), r[9:10], jnp.where(first & (index == 6), r[10:11], r))
                if k < LEVELS - 1 and TILE_LEVELS[t] > k + 1:
                    onward = jnp.where(last & (index == 8 + n), r[6 + n : 7 + n], r)
                    chain[k + 1][ch * len(tiles_of[k]) + at, LEAD - 8 : LEAD - 8 + count] = onward
                if t in TILES[k]:
                    border = jnp.where(last & (index == 8 + n), r[7 + n : 8 + n], r)
                    outs[k][ch * len(TILES[k]) + TILES[k].index(t)] = border
                    going_up, going_down = r[7:9], r[7 + n : 10 + n]
                    if t == 3:
                        going_up = jnp.where(mine, going_up, 0.0) + (up_ref[ch, 12:14] if k else 0.0)
                        going_down = jnp.where(mine, going_down, 0.0) + (down_ref[ch, 12:15] if k else 0.0)
                    up_ref[ch, 4 * t : 4 * t + 2] = going_up
                    down_ref[ch, 4 * t : 4 * t + 3] = going_down
    send_b_ref[...] = jnp.where(row_odd, down_ref[...], up_ref[...])
    send_a_ref[...] = jnp.where(row_odd, up_ref[...], down_ref[...])


def own_kernel(x_ref, t1_ref, t2_ref, t3_ref, t4_ref, t5_ref, e0, e1, e2, g0, g1, g2, g3, g4, y1, y2, y3, y4, y5):
    channels, _, height, _ = x_ref.shape
    levels, owns, ys = (t1_ref, t2_ref, t3_ref, t4_ref, t5_ref), (g0, g1, g2, g3, g4), (y1, y2, y3, y4, y5)
    for k in range(LEVELS):
        n, count, tiles = height >> (k + 1), levels[k].shape[1], len(TILES[k])
        cells = levels[k][...].reshape(channels, tiles, count, 128)
        cells = [cells[:, at].reshape(channels * count, 128) for at in range(tiles)]
        if k == 0:
            for half in range(2):
                y = times(jnp.concatenate([cells[half], cells[2]], axis=1), e0[:, 256 * half : 256 * half + 256])
                y1[:, :, 256 * half : 256 * half + 256] = y.reshape(channels, count, 256)
        elif k == 1:
            y2[...] = times(jnp.concatenate(cells, axis=1), e1[...]).reshape(y2.shape)
        else:
            ys[k][...] = times(cells[0], e2[:, 128 * (k - 2) : 128 * (k - 1)]).reshape(ys[k].shape)
        across = owns[k].shape[0] // channels
        for ch in range(channels):
            for at in range(across):
                lanes = slice(128 * at, 128 * (at + 1))
                before, center, after = (ys[k][ch, i : i + n, lanes] for i in (7, 8, 9))
                for phase, part in ((0, (before + 6.0 * center + after) * 0.125), (1, (center + after) * 0.5)):
                    if k == 0:
                        fine = x_ref[ch, at, pl.ds(phase, n, stride=2), :]
                    else:
                        fine = levels[k - 1][ch * len(TILES[k - 1]) + at, pl.ds(8 + phase, n, stride=2), :]
                    owns[k][ch * across + at, pl.ds(phase, n, stride=2), :] = fine - part


def early(row):
    return (row % 8 == 2) | ((row % 8 == 0) & (row > 0))


def end_kernel(
    g0, g1, g2, g3, g4, t5_ref, got_e_ref, got_b_ref, got_a_ref, e0, e1, e2,
    d0_hbm, d1_hbm, d2_hbm, d3_hbm, d4_hbm, coarsest_hbm,
    top0, low0, top1, low1, top2, low2, n3, n4, n5, sems,
):
    channels = got_b_ref.shape[0]
    row = lax.axis_index("rows")
    odd = row % 2 == 1
    first, last = row == 0, row == lax.axis_size("rows") - 1
    copies = []

    def out(source, target):
        copies.append(pltpu.make_async_copy(source, target, sems.at[len(copies)]))
        copies[-1].start()

    for own, hbm in ((g0, d0_hbm), (g1, d1_hbm), (g2, d2_hbm)):
        across, inner = own.shape[0] // channels, own.shape[1] - 16
        for tile in range(own.shape[0]):
            out(own.at[tile, pl.ds(8, inner)], hbm.at[tile // across, pl.ds(8, inner), pl.ds(128 * (tile % across), 128)])
    r = lax.broadcasted_iota(jnp.int32, (8, 128), 0)

    def weights(*rows):
        out = jnp.zeros((8, 128), F32)
        for at, value in rows:
            out = jnp.where(r == at, value, out)
        return out

    to_top = (weights((0, 0.125)), weights((0, 0.75), (1, 0.5), (2, 0.125)), weights((0, 0.125), (1, 0.5), (2, 0.75), (3, 0.5), (4, 0.125)))
    to_low = (weights((4, 0.125), (5, 0.5), (6, 0.75), (7, 0.5)), weights((6, 0.125), (7, 0.5)))
    coarse, fine = [[] for _ in range(4)], []
    for ch in range(channels):
        fine.append([])
        b, a = got_b_ref[ch], jnp.where(early(row - row % 2), got_e_ref[ch], got_a_ref[ch])
        from_up, from_down = jnp.where(first, 0.0, jnp.where(odd, a, b)), jnp.where(last, 0.0, jnp.where(odd, b, a))
        for t in range(4):
            up, down = from_up[4 * t : 4 * t + 3], from_down[4 * t : 4 * t + 2]
            coarse[t].append(sum(w * up[i : i + 1] for i, w in enumerate(to_top)))
            coarse[t].append(sum(w * down[i : i + 1] for i, w in enumerate(to_low)))
            fine[ch].append(
                (jnp.where(r == 0, up[1:2], jnp.where(r == 1, up[2:3], 0.0)), jnp.where(r == 7, down[:1], 0.0), down[:1])
            )
    coarse = [jnp.concatenate(tiles, axis=0) for tiles in coarse]
    e = [times(jnp.concatenate([coarse[half], coarse[3]], axis=1), e0[:, 256 * half : 256 * half + 256]) for half in range(2)]
    e.append(times(jnp.concatenate([coarse[2], coarse[3]], axis=1), e1[...]))
    e.append(times(coarse[3], e2[...]))
    for ch in range(channels):
        top, low = slice(16 * ch, 16 * ch + 8), slice(16 * ch + 8, 16 * ch + 16)
        for t in range(4):
            lanes, part = slice(128 * t, 128 * (t + 1)), e[t // 2][:, 128 * (t % 2) : 128 * (t % 2) + 128]
            top0[ch, :, lanes] = g0[4 * ch + t, :8] - part[top]
            low0[ch, :, lanes] = g0[4 * ch + t, -8:] - part[low]
        for t in range(2):
            lanes = slice(128 * t, 128 * (t + 1))
            top1[ch, :, lanes] = g1[2 * ch + t, :8] + fine[ch][t][0] - e[2][top, lanes]
            low1[ch, :, lanes] = g1[2 * ch + t, -8:] + fine[ch][t][1] - e[2][low, lanes]
        top2[ch] = g2[ch, :8] + fine[ch][2][0] - e[3][top, :128]
        low2[ch] = g2[ch, -8:] + fine[ch][2][1] - e[3][low, :128]
        n3[ch, :8] = (g3[ch, :8] + fine[ch][3][0] - e[3][top, 128:256])[:, :64]
        n3[ch, 8:] = (g3[ch, 8:] + fine[ch][3][1] - e[3][low, 128:256])[:, :64]
        n4[ch] = (g4[ch] + fine[ch][3][0] + fine[ch][3][1] - e[3][top, 256:] - e[3][low, 256:])[:, 64:96]
        n5[ch] = (t5_ref[ch, 8:16] + fine[ch][3][0] + jnp.where(r == 3, fine[ch][3][2], 0.0))[:4, 96:112]
    for top, low, hbm in ((top0, low0, d0_hbm), (top1, low1, d1_hbm), (top2, low2, d2_hbm)):
        out(top, hbm.at[:, pl.ds(0, 8)])
        out(low, hbm.at[:, pl.ds(hbm.shape[1] - 8, 8)])
    out(n3, d3_hbm)
    out(n4, d4_hbm)
    out(n5, coarsest_hbm)
    for copy in copies:
        copy.wait()


VMEM = pl.BlockSpec(memory_space=pltpu.VMEM)
HBM = pl.BlockSpec(memory_space=pltpu.HBM)


def call(kernel, outs, flops, args, scratch=(), in_space=VMEM, out_space=VMEM, limit=24 * 2**20):
    bytes_of = lambda a: a.size * a.dtype.itemsize
    outs = [jax.ShapeDtypeStruct(*(s if isinstance(s[0], tuple) else (s, F32))) for s in outs]
    return pl.pallas_call(
        kernel,
        out_shape=outs,
        in_specs=[in_space] * len(args),
        out_specs=[out_space] * len(outs),
        scratch_shapes=list(scratch),
        compiler_params=pltpu.CompilerParams(vmem_limit_bytes=limit),
        cost_estimate=pl.CostEstimate(flops=flops, bytes_accessed=sum(bytes_of(a) for a in args), transcendentals=0),
    )(*args)


def swap(x, mesh_axis, pairs, spare):
    rows, cols = lax.axis_size("rows"), lax.axis_size("cols")
    partner = dict(pairs) | {j: i for i, j in pairs}
    to = []
    for r in range(rows):
        for c in range(cols):
            if mesh_axis == "rows":
                target = (partner[r], c) if r in partner else spare(r, c)
            else:
                target = (r, partner[c]) if c in partner else spare(r, c)
            to.append(target[0] * cols + target[1])
    return lax.ppermute(x, ("rows", "cols"), list(enumerate(to)))


def body(x):
    channels, height, width = x.shape
    c = {name: jnp.asarray(value) for name, value in constants(width).items()}
    side = (channels, 16, height)
    fixed = [c[name] for name in ("edge", "col_a", "col_b", "land")]
    send_b, send_a, low, high, x_near, col_a, col_b, land = call(
        edge_kernel,
        [side] * 4 + [(channels, width // 128, height, 128)] + [(a.shape, BF16) for a in fixed[1:]],
        10**8,
        [pltpu.with_memory_space_constraint(a, pltpu.HBM) for a in (x, *fixed)],
        [pltpu.VMEM(c["edge"].shape, BF16), pltpu.SemaphoreType.DMA((8,))],
        HBM,
    )
    rows, cols = lax.axis_size("rows"), lax.axis_size("cols")
    pairs = lambda first, count: [(i, i + 1) for i in range(first, count - 1, 2)]
    got_b = swap(send_b, "cols", pairs(1, cols), lambda r, c: (r ^ 1, c))
    got_a = swap(send_a, "cols", pairs(0, cols), None)
    (u,) = call(column_kernel, [(channels, height, 512)], 10**9, (x_near, col_a, col_b))
    ns = [height >> (k + 1) for k in range(LEVELS)]
    tall = lambda tiles, n: pltpu.VMEM((tiles * channels, LEAD + n + TAIL, 128), F32)
    message = (channels, 16, 128)
    *t, send_b, send_a = call(
        row_kernel,
        [(channels * len(t), rows_of(n), 128) for n, t in zip(ns, TILES)] + [message] * 2,
        10**8,
        (u, got_b, got_a, low, high, land),
        [tall(4, height), tall(4, ns[0]), tall(2, ns[1]), tall(1, ns[2]), tall(1, ns[3])]
        + [pltpu.VMEM(message, F32)] * 2,
    )
    beside = lambda r, c: (r, c ^ 1)
    got_e = swap(send_a, "rows", [p for p in pairs(0, rows) if early(p[0])], beside)
    got_b = swap(send_b, "rows", pairs(1, rows), beside)
    got_a = swap(send_a, "rows", [p for p in pairs(0, rows) if not early(p[0])], beside)
    expand = [c[f"expand_{k}"] for k in range(3)]
    own = call(
        own_kernel,
        [(channels * max(1, width >> (k + 7)), height >> k, 128) for k in range(LEVELS)],
        10**9,
        (x_near, *t, *expand),
        [pltpu.VMEM((channels, rows_of(n), max(128, width >> k)), F32) for k, n in enumerate(ns)],
    )
    outs = [(channels, height >> k, width >> k) for k in range(LEVELS + 1)]
    return call(
        end_kernel,
        outs,
        10**8,
        (*own, t[-1], got_e, got_b, got_a, *expand),
        [pltpu.VMEM((channels, 8, s[2]), F32) for s in outs[:3] for _ in range(2)]
        + [pltpu.VMEM(s, F32) for s in outs[3:]]
        + [pltpu.SemaphoreType.DMA((30,))],
        VMEM,
        HBM,
    )


def solution(mesh):
    placed = P(None, "rows", "cols")
    return jax.shard_map(body, mesh=mesh, in_specs=(placed,), out_specs=(placed,) * 6, check_vma=False)
```

```python
import functools

import jax
import jax.numpy as jnp
import ml_dtypes
import numpy as np
from jax import lax
from jax.experimental import pallas as pl
from jax.experimental.pallas import tpu as pltpu
from jax.sharding import PartitionSpec as P


LEVELS = 5
F32 = jnp.float32
BF16 = jnp.bfloat16


def reduce_matrix(n):
    pad = np.pad(np.arange(n), (2, 2), mode="reflect")
    out = np.zeros((n // 2, n))
    for j in range(n // 2):
        for s, w in enumerate((1, 4, 6, 4, 1)):
            out[j, pad[2 * j + s]] += w / 16
    return out


def levels_of(n):
    out, total = [], np.eye(n)
    for _ in range(LEVELS):
        total = reduce_matrix(total.shape[0]) @ total
        out.append(total)
    return out


def own_rows(n, which):
    big = levels_of(5 * n)
    out = []
    for level in big:
        m = level.shape[0] // 5
        out.append(np.stack([level[2 * m + j, 2 * n : 3 * n] for j in which(m)]))
    return out


def low_fix(n):
    big, out = levels_of(3 * n), []
    for level, own in zip(big, own_rows(n, lambda m: (-1, 0, 1))):
        assert not level[:2, n:].any()
        out.append(np.stack([level[1, :n], level[0, :n], level[1, :n]]) - own)
    return out


def high_fix(n):
    big, out = levels_of(3 * n), []
    for level, own in zip(big, own_rows(n, lambda m: (m - 1, m))):
        assert not level[-1, : 2 * n].any()
        out.append(np.stack([level[-1, 2 * n :]] * 2) - own)
    return out


def expand_matrix(m):
    out = np.zeros((2 * m, m + 2))
    for i in range(m):
        out[2 * i, i : i + 3] = (0.125, 0.75, 0.125)
        out[2 * i + 1, i + 1 : i + 3] = 0.5
    return out


def exact(matrix, pieces):
    out, rest = [], np.asarray(matrix, np.float64)
    for _ in range(pieces):
        part = rest.astype(ml_dtypes.bfloat16)
        out.append(part)
        rest = rest - part.astype(np.float64)
    assert not rest.any()
    return out


OWN_LANE = (0, 256, 384, 448, 480)
LOW_LANE = tuple(496 + k for k in range(LEVELS))
HIGH_LANE = tuple(501 + k for k in range(LEVELS))
COPY_LANE = (506, 507)
TILES = ((0, 1, 3), (2, 3), (3,), (3,), (3,))
TILE_LEVELS = (1, 1, 2, 5)
LEAD = 24
TAIL = 32


def rows_of(n):
    return -(-(n + 16) // 8) * 8


@functools.lru_cache(None)
def constants(width):
    c = {}
    left = np.concatenate(own_rows(width, lambda m: (-1, 0)))
    right = np.concatenate(own_rows(width, lambda m: (m - 1, m, m + 1)))
    low, high = np.concatenate(low_fix(width)), np.concatenate(high_fix(width))
    edge = np.zeros((2, 32, 128))
    for side, at, part in ((0, 0, left), (0, 16, low), (1, 0, right), (1, 16, high)):
        near, far = (part[:, :128], part[:, 128:]) if side == 0 else (part[:, -128:], part[:, :-128])
        assert not far.any()
        edge[side, at : at + len(part)] = near
    c["edge"] = np.concatenate(exact(edge, 2), axis=1)
    own = np.zeros((width, 512))
    for k, part in enumerate(own_rows(width, lambda m: range(-1, m + 1))):
        m = part.shape[0] - 2
        own[:, OWN_LANE[k] : OWN_LANE[k] + m] = part[1:-1].T
        own[:, LOW_LANE[k]], own[:, HIGH_LANE[k]] = part[0], part[-1]
        if k == 0:
            own[:, COPY_LANE[0]], own[:, COPY_LANE[1]] = part[m // 2], part[m // 2 + 1]
    c["col_a"] = exact(own[:, :384], 1)[0]
    c["col_b"] = np.concatenate(exact(own[:, 384:], 2), axis=1)
    third = np.zeros((128, 384))
    for k in range(LEVELS):
        m = width >> (k + 1)
        e = expand_matrix(m).T
        lanes = np.zeros((512, 2 * m))
        lanes[OWN_LANE[k] : OWN_LANE[k] + m] = e[1:-1]
        lanes[LOW_LANE[k]], lanes[HIGH_LANE[k]] = e[0], e[-1]
        if k == 0:
            halves = lanes[:, :m].copy(), lanes[:, m:].copy()
            halves[0][COPY_LANE[1]], halves[1][COPY_LANE[0]] = halves[0][128], halves[1][127]
            c["expand_0"] = np.concatenate([exact(np.concatenate([halves[i][128 * i : 128 * i + 128], halves[i][384:]]), 1)[0] for i in (0, 1)], axis=1)
        elif k == 1:
            c["expand_1"] = exact(lanes[256:], 1)[0]
        else:
            at = 128 * (k - 2) + (OWN_LANE[k - 1] - 384 if k > 2 else 0)
            third[:, at : at + 2 * m] = lanes[384:]
    c["expand_2"] = exact(third, 1)[0]
    return c


def split(x):
    high = x.astype(BF16)
    rest = x - high.astype(F32)
    middle = rest.astype(BF16)
    return [high, middle, (rest - middle.astype(F32)).astype(BF16)]


def times(x, matrix):
    rows = x.shape[0]
    out = jnp.dot(jnp.concatenate(split(x), axis=0), matrix, preferred_element_type=F32)
    return out[:rows] + out[rows : 2 * rows] + out[2 * rows :]


def edge_kernel(
    x_hbm, edge_hbm, a_hbm, b_hbm,
    send_b_ref, send_a_ref, low_ref, high_ref, x_ref, a_ref, b_ref,
    edge_ref, sems,
):
    channels, height, width = x_hbm.shape
    tiles = [0, width // 128 - 1, *range(1, width // 128 - 1)]
    pairs = [(edge_hbm, edge_ref)] + [(x_hbm.at[:, :, pl.ds(128 * t, 128)], x_ref.at[:, t]) for t in tiles]
    pairs += [(a_hbm, a_ref), (b_hbm, b_ref)]
    copies = [pltpu.make_async_copy(source, target, sems.at[i]) for i, (source, target) in enumerate(pairs)]
    for copy in copies:
        copy.start()
    for copy in copies[:3]:
        copy.wait()
    odd = lax.axis_index("cols") % 2 == 1
    sides = []
    for side in range(2):
        out = sum(
            lax.dot_general(edge_ref[side], part, (((1,), (1,)), ((), ())), preferred_element_type=F32)
            for part in split(x_ref[:, tiles[side]].reshape(channels * height, 128))
        )
        sides.append(out[:32] + out[32:])
    left, right = sides
    for ch in range(channels):
        at = slice(ch * height, (ch + 1) * height)
        send_b_ref[ch] = jnp.where(odd, right[:16, at], left[:16, at])
        send_a_ref[ch] = jnp.where(odd, left[:16, at], right[:16, at])
        low_ref[ch], high_ref[ch] = left[16:, at], right[16:, at]
    for copy in copies[3:]:
        copy.wait()


def padded(ref, n):
    tiles, size = ref.shape[0], ref.shape[1]
    ref[:, :LEAD] = jnp.zeros((tiles, LEAD, 128), F32)
    ref[:, LEAD + n :] = jnp.zeros((tiles, size - LEAD - n, 128), F32)


def mirrored(ref, tile, n, first, last):
    index = lax.broadcasted_iota(jnp.int32, (8, 128), 0)
    block = ref[tile, LEAD - 8 : LEAD]
    near, far = ref[tile, LEAD + 1 : LEAD + 2], ref[tile, LEAD + 2 : LEAD + 3]
    ref[tile, LEAD - 8 : LEAD] = jnp.where(first & (index == 7), near, jnp.where(first & (index == 6), far, block))
    block = ref[tile, LEAD + n : LEAD + n + 8]
    near = ref[tile, LEAD + n - 2 : LEAD + n - 1]
    ref[tile, LEAD + n : LEAD + n + 8] = jnp.where(last & (index == 0), near, block)


def reduced(ref, tile, n, first, last):
    s = [ref[tile, pl.ds(6 + i, rows_of(n), stride=2), :] for i in range(5)]
    r = (s[0] + s[4]) * 0.0625 + (s[1] + s[3]) * 0.25 + s[2] * 0.375
    index = lax.broadcasted_iota(jnp.int32, r.shape, 0)
    r = jnp.where(first & (index == 7), r[9:10], jnp.where(first & (index == 6), r[10:11], r))
    beyond = last & (index == 8 + n)
    return jnp.where(beyond, r[6 + n : 7 + n], r), jnp.where(beyond, r[7 + n : 8 + n], r)


def column_kernel(
    x_ref, a_ref, b_ref, t1_ref, t2_ref, t3_ref, t4_ref, t5_ref, up_ref, down_ref, v_ref, c1_ref, c2_ref, c3_ref, c4_ref
):
    channels, across, height, _ = x_ref.shape
    row = lax.axis_index("rows")
    first, last = row == 0, row == lax.axis_size("rows") - 1
    chain, outs = (v_ref, c1_ref, c2_ref, c3_ref, c4_ref), (t1_ref, t2_ref, t3_ref, t4_ref, t5_ref)
    for k, ref in enumerate(chain):
        padded(ref, height >> k)
    up_ref[...] = jnp.zeros_like(up_ref)
    down_ref[...] = jnp.zeros_like(down_ref)
    x = jnp.concatenate([x_ref[:, t].reshape(channels * height, 128) for t in range(across)], axis=1)
    u = times(x, a_ref[...])
    both = times(x, b_ref[...])
    u = jnp.concatenate([u, both[:, :128] + both[:, 128:]], axis=1)
    for ch in range(channels):
        for t in range(4):
            v_ref[4 * ch + t, LEAD : LEAD + height] = u[ch * height : (ch + 1) * height, 128 * t : 128 * (t + 1)]
            mirrored(v_ref, 4 * ch + t, height, first, last)
    lane = lax.broadcasted_iota(jnp.int32, (1, 128), 1) + 384
    tiles_of = ((0, 1, 2, 3), (2, 3), (3,), (3,), (3,))
    for k in range(LEVELS):
        n = height >> (k + 1)
        count = rows_of(n)
        mine = (lane == LOW_LANE[k]) | (lane == HIGH_LANE[k])
        if k == 0:
            mine = mine | (lane == COPY_LANE[0]) | (lane == COPY_LANE[1])
        if k >= 2:
            mine = mine | (lane >= OWN_LANE[k]) & (lane < OWN_LANE[k] + (64 >> (k - 2)))
        for ch in range(channels):
            for at, t in enumerate(tiles_of[k]):
                onward, border = reduced(chain[k], ch * len(tiles_of[k]) + at, n, first, last)
                if k < LEVELS - 1 and TILE_LEVELS[t] > k + 1:
                    chain[k + 1][ch * len(tiles_of[k + 1]) + tiles_of[k + 1].index(t), LEAD - 8 : LEAD - 8 + count] = onward
                if t in TILES[k]:
                    outs[k][ch * len(TILES[k]) + TILES[k].index(t)] = border
                    going_up, going_down = border[7:9], border[7 + n : 10 + n]
                    if t == 3:
                        going_up = jnp.where(mine, going_up, 0.0) + (up_ref[ch, 12:14] if k else 0.0)
                        going_down = jnp.where(mine, going_down, 0.0) + (down_ref[ch, 12:15] if k else 0.0)
                    up_ref[ch, 4 * t : 4 * t + 2] = going_up
                    down_ref[ch, 4 * t : 4 * t + 3] = going_down


def landed(cells, k, ch, width):
    lane = lax.broadcasted_iota(jnp.int32, cells.shape, 1)
    w = width >> (k + 1)
    out = {}
    for source, target, run in (
        (3 * k, LOW_LANE[k], 1),
        (3 * k + 1, OWN_LANE[k], 2),
        (16 + 2 * k, OWN_LANE[k] + w - 1, 1),
        (17 + 2 * k, HIGH_LANE[k], 1),
    ):
        tile, at = target // 128, target % 128
        moved = pltpu.roll(cells, (at - 32 * ch - source) % 128, 1)
        out[tile] = jnp.where((lane >= at) & (lane < at + run), moved, out.get(tile, 0.0))
    return out


def row_kernel(
    got_b_ref, got_a_ref, low_ref, high_ref, own_up_ref, own_down_ref,
    send_b_ref, send_a_ref, p1_ref, p2_ref, p3_ref, p4_ref, p5_ref,
    v_ref, c1_ref, c2_ref, c3_ref, c4_ref, up_ref, down_ref,
):
    channels, height = got_b_ref.shape[0], got_b_ref.shape[2]
    col, row = lax.axis_index("cols"), lax.axis_index("rows")
    col_odd = col % 2 == 1
    row_odd, first, last = row % 2 == 1, row == 0, row == lax.axis_size("rows") - 1
    chain, outs = (v_ref, c1_ref, c2_ref, c3_ref, c4_ref), (p1_ref, p2_ref, p3_ref, p4_ref, p5_ref)
    for k, ref in enumerate(chain):
        padded(ref, height >> k)
    got = []
    for ch in range(channels):
        b, a = got_b_ref[ch], got_a_ref[ch]
        got.append(jnp.where(col == 0, low_ref[ch], jnp.where(col_odd, a, b)))
        got.append(jnp.where(col == lax.axis_size("cols") - 1, high_ref[ch], jnp.where(col_odd, b, a)))
    got.append(jnp.zeros((128 - 32 * channels, height), F32))
    v_ref[0, LEAD : LEAD + height] = jnp.concatenate(got, axis=0).T
    mirrored(v_ref, 0, height, first, last)
    up_ref[...] = own_up_ref[...]
    down_ref[...] = own_down_ref[...]
    for k in range(LEVELS):
        n = height >> (k + 1)
        onward, border = reduced(chain[k], 0, n, first, last)
        if k < LEVELS - 1:
            chain[k + 1][0, LEAD - 8 : LEAD - 8 + rows_of(n)] = onward
        outs[k][...] = border
        ends = jnp.concatenate([border[:16], border[n : n + 16]], axis=0)
        for ch in range(channels):
            for t, add in landed(ends, k, ch, 128 * 4).items():
                up_ref[ch, 4 * t : 4 * t + 2] = up_ref[ch, 4 * t : 4 * t + 2] + add[7:9]
                down_ref[ch, 4 * t : 4 * t + 3] = down_ref[ch, 4 * t : 4 * t + 3] + add[23:26]
    send_b_ref[...] = jnp.where(row_odd, down_ref[...], up_ref[...])
    send_a_ref[...] = jnp.where(row_odd, up_ref[...], down_ref[...])


def own_kernel(
    x_ref, t1_ref, t2_ref, t3_ref, t4_ref, t5_ref, p1_ref, p2_ref, p3_ref, p4_ref, p5_ref, e0, e1, e2,
    g0, g1, g2, g3, g4, s5, s1, s2, s3, s4, y1, y2, y3, y4, y5,
):
    channels, wide, height, _ = x_ref.shape
    levels, owns, ys = (s1, s2, s3, s4, s5), (g0, g1, g2, g3, g4), (y1, y2, y3, y4, y5)
    own_sums, received = (t1_ref, t2_ref, t3_ref, t4_ref, t5_ref), (p1_ref, p2_ref, p3_ref, p4_ref, p5_ref)
    for k in range(LEVELS):
        for ch in range(channels):
            add = landed(received[k][...], k, ch, 128 * wide)
            for at, t in enumerate(TILES[k]):
                tile = ch * len(TILES[k]) + at
                levels[k][tile] = own_sums[k][tile] + add[t]
        n, count, tiles = height >> (k + 1), levels[k].shape[1], len(TILES[k])
        cells = levels[k][...].reshape(channels, tiles, count, 128)
        cells = [cells[:, at].reshape(channels * count, 128) for at in range(tiles)]
        if k == 0:
            for half in range(2):
                y = times(jnp.concatenate([cells[half], cells[2]], axis=1), e0[:, 256 * half : 256 * half + 256])
                y1[:, :, 256 * half : 256 * half + 256] = y.reshape(channels, count, 256)
        elif k == 1:
            y2[...] = times(jnp.concatenate(cells, axis=1), e1[...]).reshape(y2.shape)
        else:
            ys[k][...] = times(cells[0], e2[:, 128 * (k - 2) : 128 * (k - 1)]).reshape(ys[k].shape)
        across = owns[k].shape[0] // channels
        for ch in range(channels):
            for at in range(across):
                lanes = slice(128 * at, 128 * (at + 1))
                before, center, after = (ys[k][ch, i : i + n, lanes] for i in (7, 8, 9))
                for phase, part in ((0, (before + 6.0 * center + after) * 0.125), (1, (center + after) * 0.5)):
                    if k == 0:
                        fine = x_ref[ch, at, pl.ds(phase, n, stride=2), :]
                    else:
                        fine = levels[k - 1][ch * len(TILES[k - 1]) + at, pl.ds(8 + phase, n, stride=2), :]
                    owns[k][ch * across + at, pl.ds(phase, n, stride=2), :] = fine - part


def early(row):
    return (row % 8 == 0) & (row > 0)


def end_kernel(
    g0, g1, g2, g3, g4, t5_ref, got_e_ref, got_b_ref, got_a_ref, e0, e1, e2,
    d0_hbm, d1_hbm, d2_hbm, d3_hbm, d4_hbm, coarsest_hbm,
    top0, low0, top1, low1, top2, low2, n3, n4, n5, sems,
):
    channels = got_b_ref.shape[0]
    row = lax.axis_index("rows")
    odd = row % 2 == 1
    first, last = row == 0, row == lax.axis_size("rows") - 1
    copies = []

    def out(source, target):
        copies.append(pltpu.make_async_copy(source, target, sems.at[len(copies)]))
        copies[-1].start()

    for own, hbm in ((g0, d0_hbm), (g1, d1_hbm), (g2, d2_hbm)):
        across, inner = own.shape[0] // channels, own.shape[1] - 16
        for tile in range(own.shape[0]):
            out(own.at[tile, pl.ds(8, inner)], hbm.at[tile // across, pl.ds(8, inner), pl.ds(128 * (tile % across), 128)])
    r = lax.broadcasted_iota(jnp.int32, (8, 128), 0)

    def weights(*rows):
        out = jnp.zeros((8, 128), F32)
        for at, value in rows:
            out = jnp.where(r == at, value, out)
        return out

    to_top = (weights((0, 0.125)), weights((0, 0.75), (1, 0.5), (2, 0.125)), weights((0, 0.125), (1, 0.5), (2, 0.75), (3, 0.5), (4, 0.125)))
    to_low = (weights((4, 0.125), (5, 0.5), (6, 0.75), (7, 0.5)), weights((6, 0.125), (7, 0.5)))
    coarse, fine = [[] for _ in range(4)], []
    for ch in range(channels):
        fine.append([])
        b, a = got_b_ref[ch], jnp.where(early(row - row % 2), got_e_ref[ch], got_a_ref[ch])
        from_up, from_down = jnp.where(first, 0.0, jnp.where(odd, a, b)), jnp.where(last, 0.0, jnp.where(odd, b, a))
        for t in range(4):
            up, down = from_up[4 * t : 4 * t + 3], from_down[4 * t : 4 * t + 2]
            coarse[t].append(sum(w * up[i : i + 1] for i, w in enumerate(to_top)))
            coarse[t].append(sum(w * down[i : i + 1] for i, w in enumerate(to_low)))
            fine[ch].append(
                (jnp.where(r == 0, up[1:2], jnp.where(r == 1, up[2:3], 0.0)), jnp.where(r == 7, down[:1], 0.0), down[:1])
            )
    coarse = [jnp.concatenate(tiles, axis=0) for tiles in coarse]
    e = [times(jnp.concatenate([coarse[half], coarse[3]], axis=1), e0[:, 256 * half : 256 * half + 256]) for half in range(2)]
    e.append(times(jnp.concatenate([coarse[2], coarse[3]], axis=1), e1[...]))
    e.append(times(coarse[3], e2[...]))
    for ch in range(channels):
        top, low = slice(16 * ch, 16 * ch + 8), slice(16 * ch + 8, 16 * ch + 16)
        for t in range(4):
            lanes, part = slice(128 * t, 128 * (t + 1)), e[t // 2][:, 128 * (t % 2) : 128 * (t % 2) + 128]
            top0[ch, :, lanes] = g0[4 * ch + t, :8] - part[top]
            low0[ch, :, lanes] = g0[4 * ch + t, -8:] - part[low]
        for t in range(2):
            lanes = slice(128 * t, 128 * (t + 1))
            top1[ch, :, lanes] = g1[2 * ch + t, :8] + fine[ch][t][0] - e[2][top, lanes]
            low1[ch, :, lanes] = g1[2 * ch + t, -8:] + fine[ch][t][1] - e[2][low, lanes]
        top2[ch] = g2[ch, :8] + fine[ch][2][0] - e[3][top, :128]
        low2[ch] = g2[ch, -8:] + fine[ch][2][1] - e[3][low, :128]
        n3[ch, :8] = (g3[ch, :8] + fine[ch][3][0] - e[3][top, 128:256])[:, :64]
        n3[ch, 8:] = (g3[ch, 8:] + fine[ch][3][1] - e[3][low, 128:256])[:, :64]
        n4[ch] = (g4[ch] + fine[ch][3][0] + fine[ch][3][1] - e[3][top, 256:] - e[3][low, 256:])[:, 64:96]
        n5[ch] = (t5_ref[ch, 8:16] + fine[ch][3][0] + jnp.where(r == 3, fine[ch][3][2], 0.0))[:4, 96:112]
    for top, low, hbm in ((top0, low0, d0_hbm), (top1, low1, d1_hbm), (top2, low2, d2_hbm)):
        out(top, hbm.at[:, pl.ds(0, 8)])
        out(low, hbm.at[:, pl.ds(hbm.shape[1] - 8, 8)])
    out(n3, d3_hbm)
    out(n4, d4_hbm)
    out(n5, coarsest_hbm)
    for copy in copies:
        copy.wait()


VMEM = pl.BlockSpec(memory_space=pltpu.VMEM)
HBM = pl.BlockSpec(memory_space=pltpu.HBM)


def call(kernel, outs, flops, args, scratch=(), in_space=VMEM, out_space=VMEM, limit=24 * 2**20):
    bytes_of = lambda a: a.size * a.dtype.itemsize
    outs = [jax.ShapeDtypeStruct(*(s if isinstance(s[0], tuple) else (s, F32))) for s in outs]
    return pl.pallas_call(
        kernel,
        out_shape=outs,
        in_specs=[in_space] * len(args),
        out_specs=[out_space] * len(outs),
        scratch_shapes=list(scratch),
        compiler_params=pltpu.CompilerParams(vmem_limit_bytes=limit),
        cost_estimate=pl.CostEstimate(flops=flops, bytes_accessed=sum(bytes_of(a) for a in args), transcendentals=0),
    )(*args)


def swap(x, mesh_axis, pairs, spare):
    rows, cols = lax.axis_size("rows"), lax.axis_size("cols")
    partner = dict(pairs) | {j: i for i, j in pairs}
    to = []
    for r in range(rows):
        for c in range(cols):
            if mesh_axis == "rows":
                target = (partner[r], c) if r in partner else spare(r, c)
            else:
                target = (r, partner[c]) if c in partner else spare(r, c)
            to.append(target[0] * cols + target[1])
    return lax.ppermute(x, ("rows", "cols"), list(enumerate(to)))


def body(x):
    channels, height, width = x.shape
    c = {name: jnp.asarray(value) for name, value in constants(width).items()}
    side = (channels, 16, height)
    fixed = [c[name] for name in ("edge", "col_a", "col_b")]
    send_b, send_a, low, high, x_near, col_a, col_b = call(
        edge_kernel,
        [side] * 4 + [(channels, width // 128, height, 128)] + [(a.shape, BF16) for a in fixed[1:]],
        10**8,
        [pltpu.with_memory_space_constraint(a, pltpu.HBM) for a in (x, *fixed)],
        [pltpu.VMEM(c["edge"].shape, BF16), pltpu.SemaphoreType.DMA((7,))],
        HBM,
    )
    rows, cols = lax.axis_size("rows"), lax.axis_size("cols")
    pairs = lambda first, count: [(i, i + 1) for i in range(first, count - 1, 2)]
    got_b = swap(send_b, "cols", pairs(1, cols), lambda r, c: (r ^ 1, c))
    got_a = swap(send_a, "cols", pairs(0, cols), None)
    ns = [height >> (k + 1) for k in range(LEVELS)]
    tall = lambda tiles: [pltpu.VMEM((t, LEAD + n + TAIL, 128), F32) for t, n in zip(tiles, (height, *ns))]
    message = (channels, 16, 128)
    sums = [(channels * len(t), rows_of(n), 128) for n, t in zip(ns, TILES)]
    *t, up, down = call(
        column_kernel,
        sums + [message] * 2,
        10**9,
        (x_near, col_a, col_b),
        tall([channels * count for count in (4, 2, 1, 1, 1)]),
    )
    send_b, send_a, *p = call(
        row_kernel,
        [message] * 2 + [(rows_of(n), 128) for n in ns],
        10**7,
        (got_b, got_a, low, high, up, down),
        tall([1] * 5) + [pltpu.VMEM(message, F32)] * 2,
    )
    beside = lambda r, c: (r, c ^ 1)
    got_e = swap(send_a, "rows", [p for p in pairs(0, rows) if early(p[0])], beside)
    got_b = swap(send_b, "rows", pairs(1, rows), beside)
    got_a = swap(send_a, "rows", [p for p in pairs(0, rows) if not early(p[0])], beside)
    expand = [c[f"expand_{k}"] for k in range(3)]
    *own, coarse = call(
        own_kernel,
        [(channels * max(1, width >> (k + 7)), height >> k, 128) for k in range(LEVELS)] + sums[-1:],
        10**9,
        (x_near, *t, *p, *expand),
        [pltpu.VMEM(s, F32) for s in sums[:-1]]
        + [pltpu.VMEM((channels, rows_of(n), max(128, width >> k)), F32) for k, n in enumerate(ns)],
    )
    outs = [(channels, height >> k, width >> k) for k in range(LEVELS + 1)]
    return call(
        end_kernel,
        outs,
        10**8,
        (*own, coarse, got_e, got_b, got_a, *expand),
        [pltpu.VMEM((channels, 8, s[2]), F32) for s in outs[:3] for _ in range(2)]
        + [pltpu.VMEM(s, F32) for s in outs[3:]]
        + [pltpu.SemaphoreType.DMA((30,))],
        VMEM,
        HBM,
    )


def solution(mesh):
    placed = P(None, "rows", "cols")
    return jax.shard_map(body, mesh=mesh, in_specs=(placed,), out_specs=(placed,) * 6, check_vma=False)
```

```python
import functools

import jax
import jax.numpy as jnp
import ml_dtypes
import numpy as np
from jax import lax
from jax.experimental import pallas as pl
from jax.experimental.pallas import tpu as pltpu
from jax.sharding import PartitionSpec as P


LEVELS = 5
F32 = jnp.float32
BF16 = jnp.bfloat16


def reduce_matrix(n):
    pad = np.pad(np.arange(n), (2, 2), mode="reflect")
    out = np.zeros((n // 2, n))
    for j in range(n // 2):
        for s, w in enumerate((1, 4, 6, 4, 1)):
            out[j, pad[2 * j + s]] += w / 16
    return out


def levels_of(n):
    out, total = [], np.eye(n)
    for _ in range(LEVELS):
        total = reduce_matrix(total.shape[0]) @ total
        out.append(total)
    return out


def own_rows(n, which):
    big = levels_of(5 * n)
    out = []
    for level in big:
        m = level.shape[0] // 5
        out.append(np.stack([level[2 * m + j, 2 * n : 3 * n] for j in which(m)]))
    return out


def low_fix(n):
    big, out = levels_of(3 * n), []
    for level, own in zip(big, own_rows(n, lambda m: (-1, 0, 1))):
        assert not level[:2, n:].any()
        out.append(np.stack([level[1, :n], level[0, :n], level[1, :n]]) - own)
    return out


def high_fix(n):
    big, out = levels_of(3 * n), []
    for level, own in zip(big, own_rows(n, lambda m: (m - 1, m))):
        assert not level[-1, : 2 * n].any()
        out.append(np.stack([level[-1, 2 * n :]] * 2) - own)
    return out


def expand_matrix(m):
    out = np.zeros((2 * m, m + 2))
    for i in range(m):
        out[2 * i, i : i + 3] = (0.125, 0.75, 0.125)
        out[2 * i + 1, i + 1 : i + 3] = 0.5
    return out


def exact(matrix, pieces):
    out, rest = [], np.asarray(matrix, np.float64)
    for _ in range(pieces):
        part = rest.astype(ml_dtypes.bfloat16)
        out.append(part)
        rest = rest - part.astype(np.float64)
    assert not rest.any()
    return out


OWN_LANE = (0, 256, 384, 448, 480)
LOW_LANE = tuple(496 + k for k in range(LEVELS))
HIGH_LANE = tuple(501 + k for k in range(LEVELS))
COPY_LANE = (506, 507)
TILES = ((0, 1, 3), (2, 3), (3,), (3,), (3,))
TILE_LEVELS = (1, 1, 2, 5)
MESSAGE = (32, 128)
MESSAGE_ROW = (0, 2, 4, 7)
MESSAGE_ROWS = (2, 2, 3, 3)
LEAD = 24
TAIL = 32


def rows_of(n):
    return -(-(n + 16) // 8) * 8


@functools.lru_cache(None)
def constants(width):
    c = {}
    left = np.concatenate(own_rows(width, lambda m: (-1, 0)))
    right = np.concatenate(own_rows(width, lambda m: (m - 1, m, m + 1)))
    low, high = np.concatenate(low_fix(width)), np.concatenate(high_fix(width))
    edge = np.zeros((2, 32, 128))
    for side, at, part in ((0, 0, left), (0, 16, low), (1, 0, right), (1, 16, high)):
        near, far = (part[:, :128], part[:, 128:]) if side == 0 else (part[:, -128:], part[:, :-128])
        assert not far.any()
        edge[side, at : at + len(part)] = near
    c["edge"] = np.concatenate(exact(edge, 2), axis=1)
    own = np.zeros((width, 512))
    for k, part in enumerate(own_rows(width, lambda m: range(-1, m + 1))):
        m = part.shape[0] - 2
        own[:, OWN_LANE[k] : OWN_LANE[k] + m] = part[1:-1].T
        own[:, LOW_LANE[k]], own[:, HIGH_LANE[k]] = part[0], part[-1]
        if k == 0:
            own[:, COPY_LANE[0]], own[:, COPY_LANE[1]] = part[m // 2], part[m // 2 + 1]
    c["col_a"] = exact(own[:, :384], 1)[0]
    c["col_b"] = np.concatenate(exact(own[:, 384:], 2), axis=1)
    third = np.zeros((128, 384))
    for k in range(LEVELS):
        m = width >> (k + 1)
        e = expand_matrix(m).T
        lanes = np.zeros((512, 2 * m))
        lanes[OWN_LANE[k] : OWN_LANE[k] + m] = e[1:-1]
        lanes[LOW_LANE[k]], lanes[HIGH_LANE[k]] = e[0], e[-1]
        if k == 0:
            halves = lanes[:, :m].copy(), lanes[:, m:].copy()
            halves[0][COPY_LANE[1]], halves[1][COPY_LANE[0]] = halves[0][128], halves[1][127]
            c["expand_0"] = np.concatenate([exact(np.concatenate([halves[i][128 * i : 128 * i + 128], halves[i][384:]]), 1)[0] for i in (0, 1)], axis=1)
        elif k == 1:
            c["expand_1"] = exact(lanes[256:], 1)[0]
        else:
            at = 128 * (k - 2) + (OWN_LANE[k - 1] - 384 if k > 2 else 0)
            third[:, at : at + 2 * m] = lanes[384:]
    c["expand_2"] = exact(third, 1)[0]
    return c


def split(x):
    high = x.astype(BF16)
    rest = x - high.astype(F32)
    middle = rest.astype(BF16)
    return [high, middle, (rest - middle.astype(F32)).astype(BF16)]


def times(x, matrix):
    rows = x.shape[0]
    out = jnp.dot(jnp.concatenate(split(x), axis=0), matrix, preferred_element_type=F32)
    return out[:rows] + out[rows : 2 * rows] + out[2 * rows :]


def edge_kernel(
    x_hbm, edge_hbm, a_hbm, b_hbm,
    send_b_ref, send_a_ref, low_ref, high_ref, x_ref, a_ref, b_ref,
    edge_ref, sems,
):
    channels, height, width = x_hbm.shape
    tiles = [0, width // 128 - 1, *range(1, width // 128 - 1)]
    pairs = [(edge_hbm, edge_ref)] + [(x_hbm.at[:, :, pl.ds(128 * t, 128)], x_ref.at[:, t]) for t in tiles]
    pairs += [(a_hbm, a_ref), (b_hbm, b_ref)]
    copies = [pltpu.make_async_copy(source, target, sems.at[i]) for i, (source, target) in enumerate(pairs)]
    for copy in copies:
        copy.start()
    for copy in copies[:3]:
        copy.wait()
    odd = lax.axis_index("cols") % 2 == 1
    sides = []
    for side in range(2):
        out = sum(
            lax.dot_general(edge_ref[side], part, (((1,), (1,)), ((), ())), preferred_element_type=F32)
            for part in split(x_ref[:, tiles[side]].reshape(channels * height, 128))
        )
        sides.append(out[:32] + out[32:])
    left, right = sides
    for ch in range(channels):
        at = slice(ch * height, (ch + 1) * height)
        send_b_ref[ch] = jnp.where(odd, right[:16, at], left[:16, at])
        send_a_ref[ch] = jnp.where(odd, left[:16, at], right[:16, at])
        low_ref[ch], high_ref[ch] = left[16:, at], right[16:, at]
    for copy in copies[3:]:
        copy.wait()


def padded(ref, n):
    tiles, size = ref.shape[0], ref.shape[1]
    ref[:, :LEAD] = jnp.zeros((tiles, LEAD, 128), F32)
    ref[:, LEAD + n :] = jnp.zeros((tiles, size - LEAD - n, 128), F32)


def mirrored(ref, tile, n, first, last):
    index = lax.broadcasted_iota(jnp.int32, (8, 128), 0)
    block = ref[tile, LEAD - 8 : LEAD]
    near, far = ref[tile, LEAD + 1 : LEAD + 2], ref[tile, LEAD + 2 : LEAD + 3]
    ref[tile, LEAD - 8 : LEAD] = jnp.where(first & (index == 7), near, jnp.where(first & (index == 6), far, block))
    block = ref[tile, LEAD + n : LEAD + n + 8]
    near = ref[tile, LEAD + n - 2 : LEAD + n - 1]
    ref[tile, LEAD + n : LEAD + n + 8] = jnp.where(last & (index == 0), near, block)


def reduced(ref, tile, n, first, last):
    s = [ref[tile, pl.ds(6 + i, rows_of(n), stride=2), :] for i in range(5)]
    r = (s[0] + s[4]) * 0.0625 + (s[1] + s[3]) * 0.25 + s[2] * 0.375
    index = lax.broadcasted_iota(jnp.int32, r.shape, 0)
    r = jnp.where(first & (index == 7), r[9:10], jnp.where(first & (index == 6), r[10:11], r))
    beyond = last & (index == 8 + n)
    return jnp.where(beyond, r[6 + n : 7 + n], r), jnp.where(beyond, r[7 + n : 8 + n], r)


def column_kernel(
    x_ref, a_ref, b_ref, t1_ref, t2_ref, t3_ref, t4_ref, t5_ref, up_ref, down_ref, v_ref, c1_ref, c2_ref, c3_ref, c4_ref
):
    channels, across, height, _ = x_ref.shape
    row = lax.axis_index("rows")
    first, last = row == 0, row == lax.axis_size("rows") - 1
    chain, outs = (v_ref, c1_ref, c2_ref, c3_ref, c4_ref), (t1_ref, t2_ref, t3_ref, t4_ref, t5_ref)
    for k, ref in enumerate(chain):
        padded(ref, height >> k)
    up_ref[...] = jnp.zeros_like(up_ref)
    down_ref[...] = jnp.zeros_like(down_ref)
    x = jnp.concatenate([x_ref[:, t].reshape(channels * height, 128) for t in range(across)], axis=1)
    u = times(x, a_ref[...])
    both = times(x, b_ref[...])
    u = jnp.concatenate([u, both[:, :128] + both[:, 128:]], axis=1)
    for ch in range(channels):
        for t in range(4):
            v_ref[4 * ch + t, LEAD : LEAD + height] = u[ch * height : (ch + 1) * height, 128 * t : 128 * (t + 1)]
            mirrored(v_ref, 4 * ch + t, height, first, last)
    lane = lax.broadcasted_iota(jnp.int32, (1, 128), 1) + 384
    tiles_of = ((0, 1, 2, 3), (2, 3), (3,), (3,), (3,))
    for k in range(LEVELS):
        n = height >> (k + 1)
        count = rows_of(n)
        mine = (lane == LOW_LANE[k]) | (lane == HIGH_LANE[k])
        if k == 0:
            mine = mine | (lane == COPY_LANE[0]) | (lane == COPY_LANE[1])
        if k >= 2:
            mine = mine | (lane >= OWN_LANE[k]) & (lane < OWN_LANE[k] + (64 >> (k - 2)))
        for ch in range(channels):
            for at, t in enumerate(tiles_of[k]):
                onward, border = reduced(chain[k], ch * len(tiles_of[k]) + at, n, first, last)
                if k < LEVELS - 1 and TILE_LEVELS[t] > k + 1:
                    chain[k + 1][ch * len(tiles_of[k + 1]) + tiles_of[k + 1].index(t), LEAD - 8 : LEAD - 8 + count] = onward
                if t in TILES[k]:
                    outs[k][ch * len(TILES[k]) + TILES[k].index(t)] = border
                    at_row, rows = 10 * ch + MESSAGE_ROW[t], MESSAGE_ROWS[t]
                    going_up, going_down = border[7:9], border[7 + n : 7 + n + rows]
                    if t == 3:
                        going_up = jnp.where(mine, going_up, 0.0) + (up_ref[at_row : at_row + 2] if k else 0.0)
                        going_down = jnp.where(mine, going_down, 0.0) + (down_ref[at_row : at_row + rows] if k else 0.0)
                    up_ref[at_row : at_row + 2] = going_up
                    down_ref[at_row : at_row + rows] = going_down


def landed(cells, k, ch, width, out):
    lane = lax.broadcasted_iota(jnp.int32, cells.shape, 1)
    w = width >> (k + 1)
    for source, target, run in (
        (3 * k, LOW_LANE[k], 1),
        (3 * k + 1, OWN_LANE[k], 2),
        (16 + 2 * k, OWN_LANE[k] + w - 1, 1),
        (17 + 2 * k, HIGH_LANE[k], 1),
    ):
        tile, at = target // 128, target % 128
        moved = pltpu.roll(cells, (at - 32 * ch - source) % 128, 1)
        out[tile] = jnp.where((lane >= at) & (lane < at + run), moved, out.get(tile, 0.0))
    return out


def row_kernel(
    got_b_ref, got_a_ref, low_ref, high_ref, own_up_ref, own_down_ref,
    send_b_ref, send_a_ref, p1_ref, p2_ref, p3_ref, p4_ref, p5_ref,
    v_ref, c1_ref, c2_ref, c3_ref, c4_ref, up_ref, down_ref,
):
    channels, height = got_b_ref.shape[0], got_b_ref.shape[2]
    col, row = lax.axis_index("cols"), lax.axis_index("rows")
    col_odd = col % 2 == 1
    row_odd, first, last = row % 2 == 1, row == 0, row == lax.axis_size("rows") - 1
    chain, outs = (v_ref, c1_ref, c2_ref, c3_ref, c4_ref), (p1_ref, p2_ref, p3_ref, p4_ref, p5_ref)
    for k, ref in enumerate(chain):
        padded(ref, height >> k)
    got = []
    for ch in range(channels):
        b, a = got_b_ref[ch], got_a_ref[ch]
        got.append(jnp.where(col == 0, low_ref[ch], jnp.where(col_odd, a, b)))
        got.append(jnp.where(col == lax.axis_size("cols") - 1, high_ref[ch], jnp.where(col_odd, b, a)))
    got.append(jnp.zeros((128 - 32 * channels, height), F32))
    v_ref[0, LEAD : LEAD + height] = jnp.concatenate(got, axis=0).T
    mirrored(v_ref, 0, height, first, last)
    up_ref[...] = own_up_ref[...]
    down_ref[...] = own_down_ref[...]
    r = lax.broadcasted_iota(jnp.int32, (8, 128), 0)
    tops, lows = [{} for _ in range(channels)], [{} for _ in range(channels)]
    for k in range(LEVELS):
        n = height >> (k + 1)
        onward, border = reduced(chain[k], 0, n, first, last)
        if k < LEVELS - 1:
            chain[k + 1][0, LEAD - 8 : LEAD - 8 + rows_of(n)] = onward
        outs[k][...] = border
        top = jnp.where(r == 7, border[:8], border[8:16])
        low = jnp.where(r == 7, border[n : n + 8], border[n + 8 : n + 16]) if n % 8 == 0 else pltpu.roll(border[8:16], 4, 0)
        for ch in range(channels):
            landed(top, k, ch, 128 * 4, tops[ch])
            landed(low, k, ch, 128 * 4, lows[ch])
    for ch in range(channels):
        for t in range(4):
            at, rows = 10 * ch + MESSAGE_ROW[t], MESSAGE_ROWS[t]
            up_ref[at : at + 2] = up_ref[at : at + 2] + pltpu.roll(tops[ch][t], 1, 0)[:2]
            down_ref[at : at + rows] = down_ref[at : at + rows] + pltpu.roll(lows[ch][t], 1, 0)[:rows]
    send_b_ref[...] = jnp.where(row_odd, down_ref[...], up_ref[...])
    send_a_ref[...] = jnp.where(row_odd, up_ref[...], down_ref[...])


def own_kernel(
    x_ref, t1_ref, t2_ref, t3_ref, t4_ref, t5_ref, p1_ref, p2_ref, p3_ref, p4_ref, p5_ref, e0, e1, e2,
    g0, g1, g2, g3, g4, s5, s1, s2, s3, s4, y1, y2, y3, y4, y5,
):
    channels, wide, height, _ = x_ref.shape
    levels, owns, ys = (s1, s2, s3, s4, s5), (g0, g1, g2, g3, g4), (y1, y2, y3, y4, y5)
    own_sums, received = (t1_ref, t2_ref, t3_ref, t4_ref, t5_ref), (p1_ref, p2_ref, p3_ref, p4_ref, p5_ref)
    for k in range(LEVELS):
        for ch in range(channels):
            add = landed(received[k][...], k, ch, 128 * wide, {})
            for at, t in enumerate(TILES[k]):
                tile = ch * len(TILES[k]) + at
                levels[k][tile] = own_sums[k][tile] + add[t]
        n, count, tiles = height >> (k + 1), levels[k].shape[1], len(TILES[k])
        cells = levels[k][...].reshape(channels, tiles, count, 128)
        cells = [cells[:, at].reshape(channels * count, 128) for at in range(tiles)]
        if k == 0:
            for half in range(2):
                y = times(jnp.concatenate([cells[half], cells[2]], axis=1), e0[:, 256 * half : 256 * half + 256])
                y1[:, :, 256 * half : 256 * half + 256] = y.reshape(channels, count, 256)
        elif k == 1:
            y2[...] = times(jnp.concatenate(cells, axis=1), e1[...]).reshape(y2.shape)
        else:
            ys[k][...] = times(cells[0], e2[:, 128 * (k - 2) : 128 * (k - 1)]).reshape(ys[k].shape)
        across = owns[k].shape[0] // channels
        for ch in range(channels):
            for at in range(across):
                lanes = slice(128 * at, 128 * (at + 1))
                before, center, after = (ys[k][ch, i : i + n, lanes] for i in (7, 8, 9))
                for phase, part in ((0, (before + 6.0 * center + after) * 0.125), (1, (center + after) * 0.5)):
                    if k == 0:
                        fine = x_ref[ch, at, pl.ds(phase, n, stride=2), :]
                    else:
                        fine = levels[k - 1][ch * len(TILES[k - 1]) + at, pl.ds(8 + phase, n, stride=2), :]
                    owns[k][ch * across + at, pl.ds(phase, n, stride=2), :] = fine - part


def early(row):
    return (row % 8 == 0) & (row > 0)


def end_kernel(
    g0, g1, g2, g3, g4, t5_ref, got_e_ref, got_b_ref, got_a_ref, e0, e1, e2,
    d0_hbm, d1_hbm, d2_hbm, d3_hbm, d4_hbm, coarsest_hbm,
    top0, low0, top1, low1, top2, low2, n3, n4, n5, sems,
):
    channels = n3.shape[0]
    row = lax.axis_index("rows")
    odd = row % 2 == 1
    first, last = row == 0, row == lax.axis_size("rows") - 1
    copies = []

    def out(source, target):
        copies.append(pltpu.make_async_copy(source, target, sems.at[len(copies)]))
        copies[-1].start()

    for own, hbm in ((g0, d0_hbm), (g1, d1_hbm), (g2, d2_hbm)):
        across, inner = own.shape[0] // channels, own.shape[1] - 16
        for tile in range(own.shape[0]):
            out(own.at[tile, pl.ds(8, inner)], hbm.at[tile // across, pl.ds(8, inner), pl.ds(128 * (tile % across), 128)])
    r = lax.broadcasted_iota(jnp.int32, (8, 128), 0)

    def weights(*rows):
        out = jnp.zeros((8, 128), F32)
        for at, value in rows:
            out = jnp.where(r == at, value, out)
        return out

    to_top = (weights((0, 0.125)), weights((0, 0.75), (1, 0.5), (2, 0.125)), weights((0, 0.125), (1, 0.5), (2, 0.75), (3, 0.5), (4, 0.125)))
    to_low = (weights((4, 0.125), (5, 0.5), (6, 0.75), (7, 0.5)), weights((6, 0.125), (7, 0.5)))
    coarse, fine = [[] for _ in range(4)], []
    b, a = got_b_ref[...], jnp.where(early(row - row % 2), got_e_ref[...], got_a_ref[...])
    from_up, from_down = jnp.where(first, 0.0, jnp.where(odd, a, b)), jnp.where(last, 0.0, jnp.where(odd, b, a))
    for ch in range(channels):
        fine.append([])
        for t in range(4):
            at, rows = 10 * ch + MESSAGE_ROW[t], MESSAGE_ROWS[t]
            up, down = from_up[at : at + rows], from_down[at : at + 2]
            coarse[t].append(sum(w * up[i : i + 1] for i, w in enumerate(to_top[:rows])))
            coarse[t].append(sum(w * down[i : i + 1] for i, w in enumerate(to_low)))
            top = jnp.where(r == 0, up[1:2], jnp.where(r == 1, up[2:3], 0.0) if rows > 2 else 0.0)
            fine[ch].append((top, jnp.where(r == 7, down[:1], 0.0), down[:1]))
    coarse = [jnp.concatenate(tiles, axis=0) for tiles in coarse]
    e = [times(jnp.concatenate([coarse[half], coarse[3]], axis=1), e0[:, 256 * half : 256 * half + 256]) for half in range(2)]
    e.append(times(jnp.concatenate([coarse[2], coarse[3]], axis=1), e1[...]))
    e.append(times(coarse[3], e2[...]))
    for ch in range(channels):
        top, low = slice(16 * ch, 16 * ch + 8), slice(16 * ch + 8, 16 * ch + 16)
        for t in range(4):
            lanes, part = slice(128 * t, 128 * (t + 1)), e[t // 2][:, 128 * (t % 2) : 128 * (t % 2) + 128]
            top0[ch, :, lanes] = g0[4 * ch + t, :8] - part[top]
            low0[ch, :, lanes] = g0[4 * ch + t, -8:] - part[low]
        for t in range(2):
            lanes = slice(128 * t, 128 * (t + 1))
            top1[ch, :, lanes] = g1[2 * ch + t, :8] + fine[ch][t][0] - e[2][top, lanes]
            low1[ch, :, lanes] = g1[2 * ch + t, -8:] + fine[ch][t][1] - e[2][low, lanes]
        top2[ch] = g2[ch, :8] + fine[ch][2][0] - e[3][top, :128]
        low2[ch] = g2[ch, -8:] + fine[ch][2][1] - e[3][low, :128]
        n3[ch, :8] = (g3[ch, :8] + fine[ch][3][0] - e[3][top, 128:256])[:, :64]
        n3[ch, 8:] = (g3[ch, 8:] + fine[ch][3][1] - e[3][low, 128:256])[:, :64]
        n4[ch] = (g4[ch] + fine[ch][3][0] + fine[ch][3][1] - e[3][top, 256:] - e[3][low, 256:])[:, 64:96]
        n5[ch] = (t5_ref[ch, 8:16] + fine[ch][3][0] + jnp.where(r == 3, fine[ch][3][2], 0.0))[:4, 96:112]
    for top, low, hbm in ((top0, low0, d0_hbm), (top1, low1, d1_hbm), (top2, low2, d2_hbm)):
        out(top, hbm.at[:, pl.ds(0, 8)])
        out(low, hbm.at[:, pl.ds(hbm.shape[1] - 8, 8)])
    out(n3, d3_hbm)
    out(n4, d4_hbm)
    out(n5, coarsest_hbm)
    for copy in copies:
        copy.wait()


VMEM = pl.BlockSpec(memory_space=pltpu.VMEM)
HBM = pl.BlockSpec(memory_space=pltpu.HBM)


def call(kernel, outs, flops, args, scratch=(), in_space=VMEM, out_space=VMEM, limit=24 * 2**20):
    bytes_of = lambda a: a.size * a.dtype.itemsize
    outs = [jax.ShapeDtypeStruct(*(s if isinstance(s[0], tuple) else (s, F32))) for s in outs]
    return pl.pallas_call(
        kernel,
        out_shape=outs,
        in_specs=[in_space] * len(args),
        out_specs=[out_space] * len(outs),
        scratch_shapes=list(scratch),
        compiler_params=pltpu.CompilerParams(vmem_limit_bytes=limit),
        cost_estimate=pl.CostEstimate(flops=flops, bytes_accessed=sum(bytes_of(a) for a in args), transcendentals=0),
    )(*args)


def swap(x, mesh_axis, pairs, spare):
    rows, cols = lax.axis_size("rows"), lax.axis_size("cols")
    partner = dict(pairs) | {j: i for i, j in pairs}
    to = []
    for r in range(rows):
        for c in range(cols):
            if mesh_axis == "rows":
                target = (partner[r], c) if r in partner else spare(r, c)
            else:
                target = (r, partner[c]) if c in partner else spare(r, c)
            to.append(target[0] * cols + target[1])
    return lax.ppermute(x, ("rows", "cols"), list(enumerate(to)))


def body(x):
    channels, height, width = x.shape
    c = {name: jnp.asarray(value) for name, value in constants(width).items()}
    side = (channels, 16, height)
    fixed = [c[name] for name in ("edge", "col_a", "col_b")]
    send_b, send_a, low, high, x_near, col_a, col_b = call(
        edge_kernel,
        [side] * 4 + [(channels, width // 128, height, 128)] + [(a.shape, BF16) for a in fixed[1:]],
        10**8,
        [pltpu.with_memory_space_constraint(a, pltpu.HBM) for a in (x, *fixed)],
        [pltpu.VMEM(c["edge"].shape, BF16), pltpu.SemaphoreType.DMA((7,))],
        HBM,
    )
    rows, cols = lax.axis_size("rows"), lax.axis_size("cols")
    pairs = lambda first, count: [(i, i + 1) for i in range(first, count - 1, 2)]
    got_b = swap(send_b, "cols", pairs(1, cols), lambda r, c: (r ^ 1, c))
    got_a = swap(send_a, "cols", pairs(0, cols), None)
    ns = [height >> (k + 1) for k in range(LEVELS)]
    tall = lambda tiles: [pltpu.VMEM((t, LEAD + n + TAIL, 128), F32) for t, n in zip(tiles, (height, *ns))]
    sums = [(channels * len(t), rows_of(n), 128) for n, t in zip(ns, TILES)]
    *t, up, down = call(
        column_kernel,
        sums + [MESSAGE] * 2,
        10**9,
        (x_near, col_a, col_b),
        tall([channels * count for count in (4, 2, 1, 1, 1)]),
    )
    send_b, send_a, *p = call(
        row_kernel,
        [MESSAGE] * 2 + [(rows_of(n), 128) for n in ns],
        10**7,
        (got_b, got_a, low, high, up, down),
        tall([1] * 5) + [pltpu.VMEM(MESSAGE, F32)] * 2,
    )
    beside = lambda r, c: (r, c ^ 1)
    got_e = swap(send_a, "rows", [p for p in pairs(0, rows) if early(p[0])], beside)
    got_b = swap(send_b, "rows", pairs(1, rows), beside)
    got_a = swap(send_a, "rows", [p for p in pairs(0, rows) if not early(p[0])], beside)
    expand = [c[f"expand_{k}"] for k in range(3)]
    *own, coarse = call(
        own_kernel,
        [(channels * max(1, width >> (k + 7)), height >> k, 128) for k in range(LEVELS)] + sums[-1:],
        10**9,
        (x_near, *t, *p, *expand),
        [pltpu.VMEM(s, F32) for s in sums[:-1]]
        + [pltpu.VMEM((channels, rows_of(n), max(128, width >> k)), F32) for k, n in enumerate(ns)],
    )
    outs = [(channels, height >> k, width >> k) for k in range(LEVELS + 1)]
    return call(
        end_kernel,
        outs,
        10**8,
        (*own, coarse, got_e, got_b, got_a, *expand),
        [pltpu.VMEM((channels, 8, s[2]), F32) for s in outs[:3] for _ in range(2)]
        + [pltpu.VMEM(s, F32) for s in outs[3:]]
        + [pltpu.SemaphoreType.DMA((30,))],
        VMEM,
        HBM,
    )


def solution(mesh):
    placed = P(None, "rows", "cols")
    return jax.shard_map(body, mesh=mesh, in_specs=(placed,), out_specs=(placed,) * 6, check_vma=False)
```
